32 devices in a mesh: dp: 2 (over x), ctx: 16 (over z, y, core).
Axes of the slice: x: 2, y: 2, z: 4, core: 2. Of those that a mesh axis runs over, the one named last changes fastest.
Arguments:
- queries: bfloat16 [2, 2048, 2048], P('dp', 'ctx'), may hold values from -6 to 6
- keys: bfloat16 [2, 2048, 2048], P('dp', 'ctx'), may hold values from -6 to 6
- values: bfloat16 [2, 2048, 2048], P('dp', 'ctx'), may hold values from -6 to 6
- upstream: bfloat16 [2, 2048, 2048], P('dp', 'ctx'), may hold values from -6 to 6
- filters: float32 [2048, 2048], P('ctx'), may hold values from -0.125 to 0.125
- out_weight: bfloat16 [2048, 2048], P('ctx'), may hold values from -0.125 to 0.125
Outputs:
- grad_queries: bfloat16 [2, 2048, 2048], P('dp', 'ctx')
- grad_keys: bfloat16 [2, 2048, 2048], P('dp', 'ctx')
- grad_values: bfloat16 [2, 2048, 2048], P('dp', 'ctx')
- grad_filters: float32 [2048, 2048], P('ctx')
- grad_weight: float32 [2048, 2048], P('ctx')
The draws below stay inside these ranges and needn't reach their ends.
All inputs are finite; a program needn't handle non-finite values.
Results may differ from the reference program's by a relative error of at most 0.019.
Values may be sent and summed in bfloat16 or wider, within the bound.
No kernel may reach another device: no remote copies, remote signals or barrier semaphores. Data moves between devices by JAX's collectives and lax.ppermute only.
A program may use at most 128 MiB of HBM per device.

```python
import jax
import jax.numpy as jnp
from jax import lax

C = 2048
D = 2048
SEQS = 2
SEQ_LEN = 2048


def steps_of(rng, shape, pieces, low, high):
    def one(position, parts):
        draws = jax.random.uniform(jax.random.fold_in(jax.random.fold_in(rng, 6), position), (parts,), jnp.float32, low / len(pieces), high / len(pieces))
        return jnp.repeat(jnp.exp(draws), shape[position] // parts).reshape((-1,) + (1,) * (len(shape) - position - 1))

    factor_of = one(*pieces[0])
    for cut in pieces[1:]:
        factor_of = factor_of * one(*cut)
    return factor_of


def bell_draw(key, shape, width, reach, shards=(), dtype=jnp.bfloat16):
    array = jax.random.normal(key, shape, jnp.float32) * width
    if len(shards) > 0:
        array = steps_of(key, shape, shards, -0.22, 0.18) * array
    return jnp.clip(array, min=-reach, max=reach).astype(dtype)


def setup_inputs(seed: int = 0) -> dict:
    arg_keys = jax.random.split(jax.random.key(seed), 7)
    return {
        "queries": bell_draw(arg_keys[0], (SEQS, SEQ_LEN, C), 1.0, 6.0, ((0, 2), (1, 16))),
        "keys": bell_draw(arg_keys[1], (SEQS, SEQ_LEN, C), 1.0, 6.0, ((0, 2), (1, 16))),
        "values": bell_draw(arg_keys[2], (SEQS, SEQ_LEN, C), 1.0, 6.0, ((0, 2), (1, 16))),
        "upstream": bell_draw(arg_keys[3], (SEQS, SEQ_LEN, D), 1.0, 6.0, ((0, 2), (1, 16))),
        "filters": bell_draw(arg_keys[4], (C, SEQ_LEN), SEQ_LEN ** -0.5, 0.125, ((0, 16),), jnp.float32),
        "out_weight": bell_draw(arg_keys[5], (C, D), D ** -0.5, 0.125, ((0, 16),)),
    }


def reference(queries, keys, values, upstream, filters, out_weight):
    fft_len = 2 * SEQ_LEN
    upstream_rows = upstream.reshape(SEQS * SEQ_LEN, D)
    grad_gated = jnp.dot(upstream_rows, out_weight.T, preferred_element_type=jnp.float32).astype(jnp.bfloat16)
    grad_gated = grad_gated.reshape(SEQS, SEQ_LEN, C)
    mixed_rows = (keys.astype(jnp.float32) * values.astype(jnp.float32)).astype(jnp.bfloat16)
    scaled = (grad_gated.astype(jnp.float32) * queries.astype(jnp.float32)).astype(jnp.bfloat16)
    filter_spec = jnp.fft.rfft(filters.astype(jnp.float32).T, n=fft_len, axis=0)

    def per_sequence(running, inputs):
        mixed_seq, scaled_seq = inputs
        mix_spec = jnp.fft.rfft(mixed_seq.astype(jnp.float32), n=fft_len, axis=0)
        grad_spec = jnp.fft.rfft(scaled_seq.astype(jnp.float32), n=fft_len, axis=0)
        conv_out = jnp.fft.irfft(filter_spec * mix_spec, n=fft_len, axis=0)[:SEQ_LEN]
        back_grad = jnp.fft.irfft(jnp.conj(filter_spec) * grad_spec, n=fft_len, axis=0)[:SEQ_LEN]
        filter_part = jnp.fft.irfft(jnp.conj(mix_spec) * grad_spec, n=fft_len, axis=0)[:SEQ_LEN]
        return running + filter_part.astype(jnp.float32), (conv_out.astype(jnp.bfloat16), back_grad.astype(jnp.bfloat16))

    grad_filters, outputs = lax.scan(per_sequence, jnp.zeros((SEQ_LEN, C), jnp.float32), (mixed_rows, scaled))
    conv_out, back_grad = outputs
    conv_wide = conv_out.astype(jnp.float32)
    back_wide = back_grad.astype(jnp.float32)
    grad_queries = (grad_gated.astype(jnp.float32) * conv_wide).astype(jnp.bfloat16)
    grad_keys = (back_wide * values.astype(jnp.float32)).astype(jnp.bfloat16)
    grad_values = (back_wide * keys.astype(jnp.float32)).astype(jnp.bfloat16)
    gated_rows = (queries.astype(jnp.float32) * conv_wide).astype(jnp.bfloat16).reshape(SEQS * SEQ_LEN, C)
    grad_weight = jnp.dot(gated_rows.T, upstream_rows, preferred_element_type=jnp.float32)
    return grad_queries, grad_keys, grad_values, grad_filters.T, grad_weight
```

```python
import functools
import math

import jax
import jax.numpy as jnp
import numpy as np
from jax import lax
from jax.experimental import pallas as pl
from jax.experimental.pallas import tpu as pltpu
from jax.sharding import PartitionSpec as P

INNER = 256
ROWS = 16
f32 = jnp.float32
bf16 = jnp.bfloat16


def cmul_const(z, c):
    re, im = z
    if abs(c.imag) < 1e-12:
        return (re, im) if abs(c.real - 1) < 1e-12 else (re * c.real, im * c.real)
    if abs(c.real) < 1e-12:
        if abs(c.imag - 1) < 1e-12:
            return (-im, re)
        if abs(c.imag + 1) < 1e-12:
            return (im, -re)
    return (re * c.real - im * c.imag, re * c.imag + im * c.real)


def root(n, k):
    angle = 2.0 * math.pi * (k % n) / n
    return complex(math.cos(angle), math.sin(angle))


def complex_dft(zs, sign):
    n = len(zs)
    if n == 1:
        return zs
    even = complex_dft(zs[0::2], sign)
    odd = complex_dft(zs[1::2], sign)
    turned = [cmul_const(odd[k], root(n, sign * k)) for k in range(n // 2)]
    low = [(e[0] + t[0], e[1] + t[1]) for e, t in zip(even, turned)]
    high = [(e[0] - t[0], e[1] - t[1]) for e, t in zip(even, turned)]
    return low + high


def real_dft(xs):
    n = len(xs)
    if n == 2:
        if xs[1] is None:
            return [(xs[0], None), (xs[0], None)]
        return [(xs[0] + xs[1], None), (xs[0] - xs[1], None)]
    half, quarter = n // 2, n // 4
    total = [a if b is None else a + b for a, b in zip(xs[:half], xs[half:])]
    delta = [a if b is None else a - b for a, b in zip(xs[:half], xs[half:])]
    out = [None] * (half + 1)
    for j, value in enumerate(real_dft(total)):
        out[2 * j] = value
    zs = [
        cmul_const((delta[m], -delta[m + quarter]), root(n, -m)) for m in range(quarter)
    ]
    for j, value in enumerate(complex_dft(zs, -1)):
        k = 4 * j + 1
        if k <= half:
            out[k] = value
        else:
            out[n - k] = (value[0], -value[1])
    return out


def real_inverse(zs):
    n = 2 * (len(zs) - 1)
    if n == 2:
        return [zs[0][0] + zs[1][0], zs[0][0] - zs[1][0]]
    even, odd = real_inverse(zs[0::2]), odd_part(zs)
    return [e + o for e, o in zip(even, odd)] + [e - o for e, o in zip(even, odd)]


def odd_part(zs):
    n = 2 * (len(zs) - 1)
    quarter = n // 4
    picked = []
    for j in range(quarter):
        k = 4 * j + 1
        picked.append(zs[k] if k <= n // 2 else (zs[n - k][0], -zs[n - k][1]))
    turned = [
        cmul_const(z, root(n, m)) for m, z in enumerate(complex_dft(picked, 1))
    ]
    return [2.0 * z[0] for z in turned] + [-2.0 * z[1] for z in turned]


def real_inverse_half(zs):
    return [e + o for e, o in zip(real_inverse(zs[0::2]), odd_part(zs))]


def dft_table(seq_len):
    total = 2 * seq_len
    radix = total // INNER
    k1 = np.arange(radix // 2 + 1)[:, None, None]
    k2 = np.arange(INNER)[None, :, None]
    n2 = np.arange(INNER)[None, None, :]
    angle = 2.0 * np.pi * (n2 * (k1 + radix * k2) % total) / total
    return np.stack([np.cos(angle), np.sin(angle)], axis=1).astype(jnp.bfloat16)


def dot(a, b, dims=((1,), (0,))):
    return lax.dot_general(a, b, (dims, ((), ())), preferred_element_type=f32)


def spectrum(load, table_ref, out_ref, top_ref, bot_ref):
    count = out_ref.shape[0]
    lanes = out_ref.shape[2] // 2

    def body(i, carry):
        start = pl.multiple_of(i * ROWS, ROWS)
        rows = pl.ds(start, ROWS)
        blocks = [load(n1, start) for n1 in range(count - 1)]
        for k, (re, im) in enumerate(real_dft(blocks + [None] * (count - 1))):
            re = re.astype(bf16)
            if im is None:
                top_ref[k, rows, :lanes] = re
                bot_ref[k, rows, lanes:] = -re
            else:
                im = im.astype(bf16)
                top_ref[k, rows, :lanes] = re
                top_ref[k, rows, lanes:] = im
                bot_ref[k, rows, :lanes] = im
                bot_ref[k, rows, lanes:] = -re
        return carry

    lax.fori_loop(0, INNER // ROWS, body, 0)
    for k in range(count):
        if k == 0 or k == count - 1:
            out_ref[k, :, :lanes] = dot(table_ref[k, 0], top_ref[k, :, :lanes])
            out_ref[k, :, lanes:] = dot(table_ref[k, 1], bot_ref[k, :, lanes:])
        else:
            out_ref[k] = dot(table_ref[k, 0], top_ref[k]) + dot(table_ref[k, 1], bot_ref[k])


def product_inverse(a_ref, b_ref, conj_a, table_ref, z_ref, top_ref, bot_ref, store):
    count = a_ref.shape[0]
    lanes = a_ref.shape[2] // 2
    total = 2 * (count - 1) * INNER
    for k in range(count):
        ar, ai = a_ref[k, :, :lanes], a_ref[k, :, lanes:]
        br, bi = b_ref[k, :, :lanes], b_ref[k, :, lanes:]
        if conj_a:
            re, im = ar * br + ai * bi, ar * bi - ai * br
        else:
            re, im = ar * br - ai * bi, ar * bi + ai * br
        re, im = re.astype(bf16), im.astype(bf16)
        top_ref[k, :, :lanes] = re
        bot_ref[k, :, :lanes] = -im
        if 0 < k < count - 1:
            top_ref[k, :, lanes:] = im
            bot_ref[k, :, lanes:] = re
    turn = ((0,), (0,))
    for k in range(count):
        if k == 0 or k == count - 1:
            z_ref[k, :, :lanes] = dot(table_ref[k, 0], top_ref[k, :, :lanes], turn) + dot(
                table_ref[k, 1], bot_ref[k, :, :lanes], turn
            )
        else:
            z_ref[k] = dot(table_ref[k, 0], top_ref[k], turn) + dot(
                table_ref[k, 1], bot_ref[k], turn
            )

    def body(i, carry):
        start = pl.multiple_of(i * ROWS, ROWS)
        rows = pl.ds(start, ROWS)
        zs = []
        for k in range(count):
            re = z_ref[k, rows, :lanes]
            zs.append((re, None if k in (0, count - 1) else z_ref[k, rows, lanes:]))
        for n1, value in enumerate(real_inverse_half(zs)):
            store(n1, start, value * (1.0 / total))
        return carry

    lax.fori_loop(0, INNER // ROWS, body, 0)


def filter_kernel(filters_ref, table_ref, spec_ref, turned_ref, top_ref, bot_ref):
    count = spec_ref.shape[0]
    for n1 in range(count - 1):
        turned_ref[n1] = filters_ref[:, n1 * INNER : (n1 + 1) * INNER].T
    spectrum(
        lambda n1, start: turned_ref[n1, pl.ds(start, ROWS)], table_ref, spec_ref, top_ref, bot_ref
    )


def conv_kernel(
    mixed_ref, query_ref, filt_ref, table_ref, conv_ref, gated_ref, spec_ref, z_ref, top_ref, bot_ref
):
    spectrum(
        lambda n1, start: mixed_ref[pl.ds(n1 * INNER + start, ROWS)].astype(f32),
        table_ref,
        spec_ref,
        top_ref,
        bot_ref,
    )

    def store(n1, start, value):
        rows = pl.ds(n1 * INNER + start, ROWS)
        value = value.astype(bf16)
        conv_ref[rows] = value
        gated_ref[rows] = (query_ref[rows].astype(f32) * value.astype(f32)).astype(bf16)

    product_inverse(filt_ref, spec_ref, False, table_ref, z_ref, top_ref, bot_ref, store)


def grad_kernel(n_chunks, *refs):
    chunk_refs, (weight_ref, out_ref) = refs[:n_chunks], refs[n_chunks:]
    weight = weight_ref[...]
    rows = chunk_refs[0].shape[0]
    for i, ref in enumerate(chunk_refs):
        out_ref[i * rows : (i + 1) * rows] = dot(ref[...], weight, ((1,), (1,))).astype(bf16)


def scale_kernel(n_parts, where_ref, *refs):
    part_refs, (query_ref, conv_ref, scaled_ref, out_ref) = refs[:n_parts], refs[n_parts:]
    rows = out_ref.shape[0] // where_ref.shape[0]
    i = 0
    for ref in part_refs:
        for j in range(ref.shape[0] // rows):
            place = pl.ds(pl.multiple_of(where_ref[i] * rows, rows), rows)
            grad = ref[j * rows : (j + 1) * rows].astype(f32)
            scaled_ref[place] = (grad * query_ref[place].astype(f32)).astype(bf16)
            out_ref[place] = (grad * conv_ref[place].astype(f32)).astype(bf16)
            i += 1


def back_kernel(scaled_ref, filt_ref, table_ref, back_ref, spec_ref, z_ref, top_ref, bot_ref):
    spectrum(
        lambda n1, start: scaled_ref[pl.ds(n1 * INNER + start, ROWS)].astype(f32),
        table_ref,
        spec_ref,
        top_ref,
        bot_ref,
    )

    def store(n1, start, value):
        back_ref[pl.ds(n1 * INNER + start, ROWS)] = value.astype(bf16)

    product_inverse(filt_ref, spec_ref, True, table_ref, z_ref, top_ref, bot_ref, store)


def taps_kernel(mix_ref, grad_ref, table_ref, out_ref, z_ref, top_ref, bot_ref, turned_ref):
    def store(n1, start, value):
        turned_ref[n1, pl.ds(start, ROWS)] = value

    product_inverse(mix_ref, grad_ref, True, table_ref, z_ref, top_ref, bot_ref, store)
    for n1 in range(mix_ref.shape[0] - 1):
        out_ref[:, n1 * INNER : (n1 + 1) * INNER] = turned_ref[n1].T.astype(bf16)


def weight_kernel(n_chunks, first, last, where_ref, *refs):
    chunk_refs, rest = refs[:n_chunks], refs[n_chunks:]
    gated_ref, rest = rest[0], rest[1:]
    if not first:
        sum_ref, rest = rest[0], rest[1:]
    (out_ref,) = rest
    rows = chunk_refs[0].shape[0]
    gated = [
        gated_ref[pl.ds(pl.multiple_of(where_ref[i] * rows, rows), rows)] for i in range(n_chunks)
    ]
    left = jnp.concatenate(gated, axis=0)
    width = chunk_refs[0].shape[1]
    step = 512 if width % 512 == 0 else width
    for c in range(0, width, step):
        right = jnp.concatenate([r[:, c : c + step] for r in chunk_refs], axis=0)
        acc = dot(left, right, ((0,), (0,)))
        if not first:
            acc = acc + sum_ref[:, c : c + step]
        out_ref[:, c : c + step] = acc.astype(out_ref.dtype)


def vmem():
    return pl.BlockSpec(memory_space=pltpu.VMEM)


def smem():
    return pl.BlockSpec(memory_space=pltpu.SMEM)


def call(kernel, outs, n_in, scratch=(), scalars=0, name=None, flops=0):
    return pl.pallas_call(
        kernel,
        out_shape=outs,
        in_specs=[smem()] * scalars + [vmem()] * n_in,
        out_specs=jax.tree.map(lambda _: vmem(), outs),
        scratch_shapes=list(scratch),
        name=name,
        cost_estimate=pl.CostEstimate(flops=flops, bytes_accessed=1 << 20, transcendentals=0),
    )


def chip_cycle(chips):
    rows = 1 << (chips.bit_length() // 2)
    while chips % rows:
        rows //= 2
    cols = chips // rows
    if cols == 1 or rows % 2:
        return list(range(chips))
    order = [r * cols for r in range(rows)]
    for i, r in enumerate(reversed(range(rows))):
        across = list(range(1, cols))
        order += [r * cols + c for c in (across if i % 2 == 0 else reversed(across))]
    return order


def per_device(size, queries, keys, values, upstream, filters, out_weight):
    chips = size // 2
    cycle = chip_cycle(chips)
    place = {chip: i for i, chip in enumerate(cycle)}
    forward = []
    for i, chip in enumerate(cycle):
        for core in range(2):
            forward.append((2 * chip + core, 2 * cycle[(i + 1) % chips] + core))
    backward = [(b, a) for a, b in forward]
    partner = [(i, i ^ 1) for i in range(size)]

    def sources(offset, other):
        table = []
        for p in range(size):
            chip = cycle[(place[p // 2] + offset) % chips]
            table.append(2 * chip + ((p % 2) ^ other))
        return table

    rows, queries_rows = upstream[0], queries[0]
    key_rows, value_rows = keys[0], values[0]
    local_t, width = rows.shape
    chan = out_weight.shape[0]
    seq_len = filters.shape[1]
    count = seq_len // INNER + 1
    table = jnp.asarray(dft_table(seq_len))
    spec = jax.ShapeDtypeStruct((count, INNER, 2 * chan), f32)
    chan_bf = jax.ShapeDtypeStruct((seq_len, chan), bf16)
    top = pltpu.VMEM((count, INNER, 2 * chan), bf16)
    zs = pltpu.VMEM((count, INNER, 2 * chan), f32)
    turned = pltpu.VMEM((count - 1, INNER, chan), f32)
    one = 8 * count * INNER * INNER * chan

    def to_chan(x):
        x = x.reshape(local_t, size, chan).transpose(1, 0, 2)
        return lax.all_to_all(x, "ctx", 0, 0, tiled=True).reshape(seq_len, chan)

    def to_token(x):
        x = lax.all_to_all(x.reshape(size, local_t, chan), "ctx", 0, 0, tiled=True)
        return x.transpose(1, 0, 2).reshape(local_t, size * chan)

    mixed_rows = (key_rows.astype(f32) * value_rows.astype(f32)).astype(bf16)

    groups = [[(rows, 0, 0), (lax.ppermute(rows, "ctx", partner), 0, 1)]]
    ahead, behind = rows, rows
    for step in range(1, chips // 2 + 1):
        group = []
        ahead = lax.ppermute(ahead, "ctx", forward)
        group += [(ahead, -step, 0), (lax.ppermute(ahead, "ctx", partner), -step, 1)]
        if step <= (chips - 1) // 2:
            behind = lax.ppermute(behind, "ctx", backward)
            group += [(behind, step, 0), (lax.ppermute(behind, "ctx", partner), step, 1)]
        groups.append(group)

    filt_spec = call(filter_kernel, spec, 2, [turned, top, top], name="filter_spec", flops=one)(
        filters, table
    )
    mixed_chan, query_chan = to_chan(mixed_rows), to_chan(queries_rows)
    conv_chan, gated_chan, mix_spec = call(
        conv_kernel,
        (chan_bf, chan_bf, spec),
        4,
        [zs, top, top],
        name="conv",
        flops=2 * one,
    )(mixed_chan, query_chan, filt_spec, table)

    me = lax.axis_index("ctx")
    parts, where = [], []
    for i, group in enumerate(groups):
        n = len(group)
        parts.append(
            call(
                functools.partial(grad_kernel, n),
                jax.ShapeDtypeStruct((n * local_t, chan), bf16),
                n + 1,
                name=f"grad_{i}",
                flops=2 * n * local_t * width * chan,
            )(*[g[0] for g in group], out_weight)
        )
        where += [sources(g[1], g[2]) for g in group]
    where = jnp.asarray(np.array(where, np.int32).T)[me]

    scaled, queries_chan = call(
        functools.partial(scale_kernel, len(parts)),
        (chan_bf, chan_bf),
        len(parts) + 2,
        scalars=1,
        name="scale",
        flops=seq_len * chan,
    )(where, *parts, query_chan, conv_chan)
    grad_queries = to_token(queries_chan)

    back_chan, grad_spec = call(
        back_kernel, (chan_bf, spec), 3, [zs, top, top], name="back", flops=2 * one
    )(scaled, filt_spec, table)
    back_wide = to_token(back_chan).astype(f32)
    grad_keys = (back_wide * value_rows.astype(f32)).astype(bf16)
    grad_values = (back_wide * key_rows.astype(f32)).astype(bf16)

    taps = call(
        taps_kernel,
        jax.ShapeDtypeStruct((chan, seq_len), bf16),
        3,
        [zs, top, top, turned],
        name="taps",
        flops=one,
    )(mix_spec, grad_spec, table)

    first = [g[0] for group in groups[:-1] for g in group]
    final = [g[0] for g in groups[-1]]
    total = call(
        functools.partial(weight_kernel, len(first), True, False),
        jax.ShapeDtypeStruct((chan, width), f32),
        len(first) + 1,
        scalars=1,
        name="weight_first",
        flops=2 * len(first) * local_t * width * chan,
    )(where[: len(first)], *first, gated_chan)
    part_weight = call(
        functools.partial(weight_kernel, len(final), False, True),
        jax.ShapeDtypeStruct((chan, width), bf16),
        len(final) + 2,
        scalars=1,
        name="weight_last",
        flops=2 * len(final) * local_t * width * chan,
    )(where[len(first) :], *final, gated_chan, total)

    def over_dp(x):
        n = lax.axis_size("dp")
        total = x.astype(f32)
        if n == 2:
            return total + lax.ppermute(x, "dp", [(0, 1), (1, 0)]).astype(f32)
        return lax.psum(x, "dp").astype(f32)

    return (
        grad_queries[None],
        grad_keys[None],
        grad_values[None],
        over_dp(taps),
        over_dp(part_weight),
    )


def solution(mesh):
    tokens, chans = P("dp", "ctx", None), P("ctx", None)
    return jax.shard_map(
        functools.partial(per_device, mesh.shape["ctx"]),
        mesh=mesh,
        in_specs=(tokens, tokens, tokens, tokens, chans, chans),
        out_specs=(tokens, tokens, tokens, chans, chans),
        check_vma=False,
    )
```

```python
import functools
import math

import jax
import jax.numpy as jnp
import numpy as np
from jax import lax
from jax.experimental import pallas as pl
from jax.experimental.pallas import tpu as pltpu
from jax.sharding import PartitionSpec as P


INNER = 256
ROWS = 16
VMEM_LIMIT = 20 << 20
f32 = jnp.float32
bf16 = jnp.bfloat16


def cmul_const(z, c):
    re, im = z
    if abs(c.imag) < 1e-12:
        return (re, im) if abs(c.real - 1) < 1e-12 else (re * c.real, im * c.real)
    if abs(c.real) < 1e-12:
        if abs(c.imag - 1) < 1e-12:
            return (-im, re)
        if abs(c.imag + 1) < 1e-12:
            return (im, -re)
    return (re * c.real - im * c.imag, re * c.imag + im * c.real)


def root(n, k):
    angle = 2.0 * math.pi * (k % n) / n
    return complex(math.cos(angle), math.sin(angle))


def complex_dft(zs, sign):
    n = len(zs)
    if n == 1:
        return zs
    even = complex_dft(zs[0::2], sign)
    odd = complex_dft(zs[1::2], sign)
    turned = [cmul_const(odd[k], root(n, sign * k)) for k in range(n // 2)]
    low = [(e[0] + t[0], e[1] + t[1]) for e, t in zip(even, turned)]
    high = [(e[0] - t[0], e[1] - t[1]) for e, t in zip(even, turned)]
    return low + high


def real_dft(xs):
    n = len(xs)
    if n == 2:
        if xs[1] is None:
            return [(xs[0], None), (xs[0], None)]
        return [(xs[0] + xs[1], None), (xs[0] - xs[1], None)]
    half, quarter = n // 2, n // 4
    total = [a if b is None else a + b for a, b in zip(xs[:half], xs[half:])]
    delta = [a if b is None else a - b for a, b in zip(xs[:half], xs[half:])]
    out = [None] * (half + 1)
    for j, value in enumerate(real_dft(total)):
        out[2 * j] = value
    zs = [
        cmul_const((delta[m], -delta[m + quarter]), root(n, -m)) for m in range(quarter)
    ]
    for j, value in enumerate(complex_dft(zs, -1)):
        k = 4 * j + 1
        if k <= half:
            out[k] = value
        else:
            out[n - k] = (value[0], -value[1])
    return out


def real_inverse(zs):
    n = 2 * (len(zs) - 1)
    if n == 2:
        return [zs[0][0] + zs[1][0], zs[0][0] - zs[1][0]]
    even, odd = real_inverse(zs[0::2]), odd_part(zs)
    return [e + o for e, o in zip(even, odd)] + [e - o for e, o in zip(even, odd)]


def odd_part(zs):
    n = 2 * (len(zs) - 1)
    quarter = n // 4
    picked = []
    for j in range(quarter):
        k = 4 * j + 1
        picked.append(zs[k] if k <= n // 2 else (zs[n - k][0], -zs[n - k][1]))
    turned = [
        cmul_const(z, root(n, m)) for m, z in enumerate(complex_dft(picked, 1))
    ]
    return [2.0 * z[0] for z in turned] + [-2.0 * z[1] for z in turned]


def real_inverse_half(zs):
    return [e + o for e, o in zip(real_inverse(zs[0::2]), odd_part(zs))]


def dft_table(seq_len):
    total = 2 * seq_len
    radix = total // INNER
    k1 = np.arange(radix // 2 + 1)[:, None, None]
    k2 = np.arange(INNER)[None, :, None]
    n2 = np.arange(INNER)[None, None, :]
    angle = 2.0 * np.pi * (n2 * (k1 + radix * k2) % total) / total
    return np.stack([np.cos(angle), np.sin(angle)], axis=1).astype(jnp.bfloat16)


def dot(a, b, dims=((1,), (0,))):
    return lax.dot_general(a, b, (dims, ((), ())), preferred_element_type=f32)


def spectrum(load, table_ref, out_ref, top_ref, bot_ref, saved=None):
    copies = []
    count = out_ref.shape[0]
    lanes = out_ref.shape[2] // 2

    def body(i, carry):
        start = pl.multiple_of(i * ROWS, ROWS)
        rows = pl.ds(start, ROWS)
        blocks = [load(n1, start) for n1 in range(count - 1)]
        for k, (re, im) in enumerate(real_dft(blocks + [None] * (count - 1))):
            re = re.astype(bf16)
            if im is None:
                top_ref[k, rows, :lanes] = re
                bot_ref[k, rows, lanes:] = -re
            else:
                im = im.astype(bf16)
                top_ref[k, rows, :lanes] = re
                top_ref[k, rows, lanes:] = im
                bot_ref[k, rows, :lanes] = im
                bot_ref[k, rows, lanes:] = -re
        return carry

    lax.fori_loop(0, INNER // ROWS, body, 0)
    for k in range(count):
        if k == 0 or k == count - 1:
            out_ref[k, :, :lanes] = dot(table_ref[k, 0], top_ref[k, :, :lanes])
            out_ref[k, :, lanes:] = dot(table_ref[k, 1], bot_ref[k, :, lanes:])
        else:
            out_ref[k] = dot(table_ref[k, 0], top_ref[k]) + dot(table_ref[k, 1], bot_ref[k])
        if saved is not None:
            copies.append(pltpu.make_async_copy(out_ref.at[k], saved[0].at[k], saved[1].at[k]))
            copies[-1].start()
    return copies


def product_inverse(a_ref, b_ref, conj_a, table_ref, z_ref, top_ref, bot_ref, store):
    count = a_ref.shape[0]
    lanes = a_ref.shape[2] // 2
    total = 2 * (count - 1) * INNER
    for k in range(count):
        ar, ai = a_ref[k, :, :lanes], a_ref[k, :, lanes:]
        br, bi = b_ref[k, :, :lanes], b_ref[k, :, lanes:]
        if conj_a:
            re, im = ar * br + ai * bi, ar * bi - ai * br
        else:
            re, im = ar * br - ai * bi, ar * bi + ai * br
        re, im = re.astype(bf16), im.astype(bf16)
        top_ref[k, :, :lanes] = re
        bot_ref[k, :, :lanes] = -im
        if 0 < k < count - 1:
            top_ref[k, :, lanes:] = im
            bot_ref[k, :, lanes:] = re
    turn = ((0,), (0,))
    for k in range(count):
        if k == 0 or k == count - 1:
            z_ref[k, :, :lanes] = dot(table_ref[k, 0], top_ref[k, :, :lanes], turn) + dot(
                table_ref[k, 1], bot_ref[k, :, :lanes], turn
            )
        else:
            z_ref[k] = dot(table_ref[k, 0], top_ref[k], turn) + dot(
                table_ref[k, 1], bot_ref[k], turn
            )

    def body(i, carry):
        start = pl.multiple_of(i * ROWS, ROWS)
        rows = pl.ds(start, ROWS)
        zs = []
        for k in range(count):
            re = z_ref[k, rows, :lanes]
            zs.append((re, None if k in (0, count - 1) else z_ref[k, rows, lanes:]))
        for n1, value in enumerate(real_inverse_half(zs)):
            store(n1, start, value * (1.0 / total))
        return carry

    lax.fori_loop(0, INNER // ROWS, body, 0)


def filter_kernel(filters_ref, table_ref, saved_ref, spec_ref, turned_ref, top_ref, bot_ref, sems):
    count = spec_ref.shape[0]
    for n1 in range(count - 1):
        turned_ref[n1] = filters_ref[:, n1 * INNER : (n1 + 1) * INNER].T
    for copy in spectrum(
        lambda n1, start: turned_ref[n1, pl.ds(start, ROWS)],
        table_ref,
        spec_ref,
        top_ref,
        bot_ref,
        (saved_ref, sems),
    ):
        copy.wait()


def conv_kernel(
    got_ref,
    filters_ref,
    table_ref,
    conv_ref,
    gated_ref,
    saved_ref,
    filt_ref,
    spec_ref,
    z_ref,
    top_ref,
    bot_ref,
    sems,
    sem,
):
    local_t = got_ref.shape[2]
    fetch = pltpu.make_async_copy(filters_ref, filt_ref, sem)
    fetch.start()

    def load(kind, token):
        here = pl.ds(pl.multiple_of(token % local_t, ROWS), ROWS)
        return got_ref[token // local_t, kind, here].astype(f32)

    copies = spectrum(
        lambda n1, start: load(0, n1 * INNER + start),
        table_ref,
        spec_ref,
        top_ref,
        bot_ref,
        (saved_ref, sems),
    )
    fetch.wait()

    def store(n1, start, value):
        rows = pl.ds(n1 * INNER + start, ROWS)
        value = value.astype(bf16)
        conv_ref[rows] = value
        query = load(1, n1 * INNER + start)
        gated_ref[rows] = (query * value.astype(f32)).astype(bf16)

    product_inverse(filt_ref, spec_ref, False, table_ref, z_ref, top_ref, bot_ref, store)
    for copy in copies:
        copy.wait()


def grad_kernel(n_chunks, *refs):
    chunk_refs, (weight_ref, out_ref, rows_ref) = refs[:n_chunks], refs[n_chunks:]
    rows = chunk_refs[0].shape[0]
    for i, ref in enumerate(chunk_refs):
        rows_ref[i * rows : (i + 1) * rows] = ref[...]
    out_ref[...] = dot(rows_ref[...], weight_ref[...], ((1,), (1,))).astype(bf16)


def split_kernel(key_ref, value_ref, query_ref, out_ref):
    n, _, _, chan = out_ref.shape
    for p in range(n):
        cols = slice(p * chan, (p + 1) * chan)
        mixed = key_ref[:, cols].astype(f32) * value_ref[:, cols].astype(f32)
        out_ref[p, 0] = mixed.astype(bf16)
        out_ref[p, 1] = query_ref[:, cols]


def finish_kernel(got_ref, key_ref, value_ref, grad_query_ref, grad_key_ref, grad_value_ref):
    n, _, _, chan = got_ref.shape
    for p in range(n):
        cols = slice(p * chan, (p + 1) * chan)
        grad_query_ref[:, cols] = got_ref[p, 0]
        back = got_ref[p, 1].astype(f32)
        grad_key_ref[:, cols] = (back * value_ref[:, cols].astype(f32)).astype(bf16)
        grad_value_ref[:, cols] = (back * key_ref[:, cols].astype(f32)).astype(bf16)


def tail_kernel(n_parts, n_chunks, where_ref, *refs):
    part_refs, refs = refs[:n_parts], refs[n_parts:]
    chunk_refs, refs = refs[:n_chunks], refs[n_chunks:]
    weight_ref, got_ref, conv_ref, filters_ref, table_ref, *refs = refs
    out_ref, saved_ref, scaled_ref, rows_ref, grad_ref, *refs = refs
    filt_ref, spec_ref, z_ref, top_ref, bot_ref, sems, sem = refs
    fetch = pltpu.make_async_copy(filters_ref, filt_ref, sem)
    fetch.start()
    rows = chunk_refs[0].shape[0]
    _, _, local_t, _ = out_ref.shape
    halves = local_t // rows
    weight = weight_ref[...]
    i = 0

    def scale(grad, unit):
        block, start = unit // halves, pl.multiple_of(unit % halves * rows, rows)
        here, place = pl.ds(start, rows), pl.ds(pl.multiple_of(unit * rows, rows), rows)
        query = got_ref[block, 1, here].astype(f32)
        scaled_ref[place] = (grad * query).astype(bf16)
        out_ref[block, 0, here] = (grad * conv_ref[place].astype(f32)).astype(bf16)

    for ref in part_refs:
        for j in range(ref.shape[0] // rows):
            scale(ref[j * rows : (j + 1) * rows].astype(f32), where_ref[i])
            i += 1
    for j, ref in enumerate(chunk_refs):
        rows_ref[j * rows : (j + 1) * rows] = ref[...]
    grad_ref[...] = dot(rows_ref[...], weight, ((1,), (1,))).astype(bf16)
    for j in range(n_chunks):
        scale(grad_ref[j * rows : (j + 1) * rows].astype(f32), where_ref[i + j])
    copies = spectrum(
        lambda n1, start: scaled_ref[pl.ds(n1 * INNER + start, ROWS)].astype(f32),
        table_ref,
        spec_ref,
        top_ref,
        bot_ref,
        (saved_ref, sems),
    )
    fetch.wait()

    def store(n1, start, value):
        token = n1 * INNER + start
        here = pl.ds(pl.multiple_of(token % local_t, ROWS), ROWS)
        out_ref[token // local_t, 1, here] = value.astype(bf16)

    product_inverse(filt_ref, spec_ref, True, table_ref, z_ref, top_ref, bot_ref, store)
    for copy in copies:
        copy.wait()


def taps_kernel(
    saved_mix, saved_grad, table_ref, out_ref, mix_ref, grad_ref, z_ref, top_ref, bot_ref, turned_ref, sems
):
    fetch = [
        pltpu.make_async_copy(saved_mix, mix_ref, sems.at[0]),
        pltpu.make_async_copy(saved_grad, grad_ref, sems.at[1]),
    ]
    for copy in fetch:
        copy.start()
    for copy in fetch:
        copy.wait()

    def store(n1, start, value):
        turned_ref[n1, pl.ds(start, ROWS)] = value

    product_inverse(mix_ref, grad_ref, True, table_ref, z_ref, top_ref, bot_ref, store)
    for n1 in range(mix_ref.shape[0] - 1):
        out_ref[:, n1 * INNER : (n1 + 1) * INNER] = turned_ref[n1].T.astype(bf16)


def weight_kernel(n_chunks, first, unit, where_ref, *refs):
    chunk_refs, rest = refs[:n_chunks], refs[n_chunks:]
    gated_ref, rest = rest[0], rest[1:]
    if not first:
        sum_ref, rest = rest[0], rest[1:]
    (out_ref,) = rest
    gated, i = [], 0
    for ref in chunk_refs:
        for _ in range(ref.shape[0] // unit):
            gated.append(gated_ref[pl.ds(pl.multiple_of(where_ref[i] * unit, unit), unit)])
            i += 1
    left = jnp.concatenate(gated, axis=0)
    width = chunk_refs[0].shape[1]
    step = 512 if width % 512 == 0 else width
    for c in range(0, width, step):
        right = jnp.concatenate([r[:, c : c + step] for r in chunk_refs], axis=0)
        acc = dot(left, right, ((0,), (0,)))
        if not first:
            acc = acc + sum_ref[:, c : c + step]
        out_ref[:, c : c + step] = acc.astype(out_ref.dtype)


def vmem():
    return pl.BlockSpec(memory_space=pltpu.VMEM)


def hbm():
    return pl.BlockSpec(memory_space=pltpu.HBM)


def smem():
    return pl.BlockSpec(memory_space=pltpu.SMEM)


def in_hbm(x):
    return pltpu.with_memory_space_constraint(x, pltpu.HBM)


def call(kernel, outs, n_in, scratch=(), scalars=0, flops=0, kept=(), saved=None):
    ins = [hbm() if i in kept else vmem() for i in range(n_in)]
    many = isinstance(outs, tuple)
    specs = [hbm() if i == saved else vmem() for i in range(len(outs) if many else 1)]
    return pl.pallas_call(
        kernel,
        out_shape=outs,
        in_specs=[smem()] * scalars + ins,
        out_specs=tuple(specs) if many else specs[0],
        scratch_shapes=list(scratch),
        compiler_params=pltpu.CompilerParams(vmem_limit_bytes=VMEM_LIMIT),
        cost_estimate=pl.CostEstimate(flops=flops, bytes_accessed=1 << 20, transcendentals=0),
    )


def chip_cycle(chips):
    rows = 1 << (chips.bit_length() // 2)
    while chips % rows:
        rows //= 2
    cols = chips // rows
    if cols == 1 or rows % 2:
        return list(range(chips))
    order = [r * cols for r in range(rows)]
    for i, r in enumerate(reversed(range(rows))):
        across = list(range(1, cols))
        order += [r * cols + c for c in (across if i % 2 == 0 else reversed(across))]
    return order


def per_device(size, queries, keys, values, upstream, filters, out_weight):
    chips = size // 2
    cycle = chip_cycle(chips)
    place = {chip: i for i, chip in enumerate(cycle)}
    forward = []
    for i, chip in enumerate(cycle):
        for core in range(2):
            forward.append((2 * chip + core, 2 * cycle[(i + 1) % chips] + core))
    backward = [(b, a) for a, b in forward]
    partner = [(i, i ^ 1) for i in range(size)]

    def sources(offset, other):
        table = []
        for p in range(size):
            chip = cycle[(place[p // 2] + offset) % chips]
            table.append(2 * chip + ((p % 2) ^ other))
        return table

    rows, queries_rows = upstream[0], queries[0]
    key_rows, value_rows = keys[0], values[0]
    local_t, width = rows.shape
    chan = out_weight.shape[0]
    seq_len = filters.shape[1]
    count = seq_len // INNER + 1
    table = jnp.asarray(dft_table(seq_len))
    spec = pltpu.HBM((count, INNER, 2 * chan), f32)
    chan_bf = pltpu.HBM((seq_len, chan), bf16)
    sem, sems = pltpu.SemaphoreType.DMA(()), pltpu.SemaphoreType.DMA((count,))
    top = pltpu.VMEM((count, INNER, 2 * chan), bf16)
    zs = pltpu.VMEM((count, INNER, 2 * chan), f32)
    turned = pltpu.VMEM((count - 1, INNER, chan), f32)
    one = 8 * count * INNER * INNER * chan

    half = local_t // 2
    steps = chips // 2
    me = lax.axis_index("ctx")

    def to_partner(x):
        return lax.ppermute(x, "ctx", partner)

    def exchange(x):
        return lax.all_to_all(x, "ctx", 0, 0, tiled=True)

    def grad_of(group):
        n = len(group)
        return call(
            functools.partial(grad_kernel, n),
            pltpu.HBM((n * local_t, chan), bf16),
            n + 1,
            [pltpu.VMEM((n * local_t, width), bf16)],
            flops=2 * n * local_t * width * chan,
        )(*[g[0] for g in group], out_weight)

    def pair(x, offset, halves=(0, 1)):
        return [(x, offset, 0, halves), (to_partner(x), offset, 1, halves)]

    blocks = pltpu.HBM((size, 2, local_t, chan), bf16)
    send = call(split_kernel, blocks, 3, flops=seq_len * chan)(
        in_hbm(key_rows), in_hbm(value_rows), in_hbm(queries_rows)
    )
    got = exchange(send)
    filt_spec = call(filter_kernel, spec, 2, [zs, turned, top, top, sems], flops=one, saved=0)(
        in_hbm(filters), table
    )
    groups = [pair(rows, 0)]
    parts = []
    ahead, behind = rows, rows
    for step in range(1, steps):
        ahead = lax.ppermute(ahead, "ctx", forward)
        behind = lax.ppermute(behind, "ctx", backward)
        groups.append(pair(ahead, -step) + pair(behind, step))
        parts.append(grad_of(groups[step - 1]))
    ahead = lax.ppermute(ahead[:half], "ctx", forward)
    behind = lax.ppermute(behind[half:], "ctx", backward)
    parts.append(grad_of(groups[-1]))
    conv_chan, gated_chan, mix_spec = call(
        conv_kernel,
        (chan_bf, chan_bf, spec),
        3,
        [zs, zs, zs, top, top, sems, sem],
        flops=2 * one,
        kept=(1,),
        saved=2,
    )(got, in_hbm(filt_spec), table)
    groups.append(pair(ahead, -steps, (0,)) + pair(behind, -steps, (1,)))

    where = [[2 * p + h for p in sources(g[1], g[2])] for group in groups for g in group for h in g[3]]
    where = jnp.asarray(np.array(where, np.int32).T)[me]

    first = [g[0] for group in groups[:-1] for g in group]
    final = [g[0] for g in groups[-1]]
    total = call(
        functools.partial(weight_kernel, len(first), True, half),
        pltpu.VMEM((chan, width), f32),
        len(first) + 1,
        scalars=1,
        flops=2 * len(first) * local_t * width * chan,
    )(where[: -len(final)], *first, gated_chan)

    back, grad_spec = call(
        functools.partial(tail_kernel, len(parts), len(final)),
        (blocks, spec),
        len(parts) + len(final) + 5,
        [
            pltpu.VMEM((seq_len, chan), bf16),
            pltpu.VMEM((len(final) * half, width), bf16),
            pltpu.VMEM((len(final) * half, chan), bf16),
            zs,
            zs,
            zs,
            top,
            top,
            sems,
            sem,
        ],
        scalars=1,
        flops=2 * one,
        kept=(len(parts) + len(final) + 3,),
        saved=1,
    )(where, *parts, *final, out_weight, got, conv_chan, in_hbm(filt_spec), table)
    back = exchange(back)

    part_weight = call(
        functools.partial(weight_kernel, len(final), False, half),
        jax.ShapeDtypeStruct((chan, width), bf16),
        len(final) + 2,
        scalars=1,
        flops=2 * len(final) * half * width * chan,
    )(where[-len(final) :], *final, gated_chan, total)
    taps = call(
        taps_kernel,
        jax.ShapeDtypeStruct((chan, seq_len), bf16),
        3,
        [zs, zs, zs, top, top, turned, pltpu.SemaphoreType.DMA((2,))],
        flops=one,
        kept=(0, 1),
    )(in_hbm(mix_spec), in_hbm(grad_spec), table)
    rows_bf = jax.ShapeDtypeStruct((local_t, size * chan), bf16)
    grad_queries, grad_keys, grad_values = call(
        finish_kernel, (rows_bf, rows_bf, rows_bf), 3, flops=seq_len * chan
    )(back, key_rows, value_rows)

    def over_dp(x):
        n = lax.axis_size("dp")
        total = x.astype(f32)
        if n == 2:
            return total + lax.ppermute(x, "dp", [(0, 1), (1, 0)]).astype(f32)
        return lax.psum(x, "dp").astype(f32)

    return (
        grad_queries[None], grad_keys[None], grad_values[None], over_dp(taps), over_dp(part_weight)
    )


def solution(mesh):
    tokens, chans = P("dp", "ctx", None), P("ctx", None)

    def body(*args):
        return per_device(mesh.shape["ctx"], *args)

    return jax.shard_map(
        body,
        mesh=mesh,
        in_specs=(tokens, tokens, tokens, tokens, chans, chans),
        out_specs=(tokens, tokens, tokens, chans, chans),
        check_vma=False,
    )
```

```python
import functools
import math

import jax
import jax.numpy as jnp
import numpy as np
from jax import lax
from jax.experimental import pallas as pl
from jax.experimental.pallas import tpu as pltpu
from jax.sharding import PartitionSpec as P


INNER = 256
ROWS = 16
VMEM_LIMIT = 20 << 20
f32 = jnp.float32
bf16 = jnp.bfloat16


def cmul_const(z, c):
    re, im = z
    if abs(c.imag) < 1e-12:
        return (re, im) if abs(c.real - 1) < 1e-12 else (re * c.real, im * c.real)
    if abs(c.real) < 1e-12:
        if abs(c.imag - 1) < 1e-12:
            return (-im, re)
        if abs(c.imag + 1) < 1e-12:
            return (im, -re)
    return (re * c.real - im * c.imag, re * c.imag + im * c.real)


def root(n, k):
    angle = 2.0 * math.pi * (k % n) / n
    return complex(math.cos(angle), math.sin(angle))


def complex_dft(zs, sign):
    n = len(zs)
    if n == 1:
        return zs
    even = complex_dft(zs[0::2], sign)
    odd = complex_dft(zs[1::2], sign)
    turned = [cmul_const(odd[k], root(n, sign * k)) for k in range(n // 2)]
    low = [(e[0] + t[0], e[1] + t[1]) for e, t in zip(even, turned)]
    high = [(e[0] - t[0], e[1] - t[1]) for e, t in zip(even, turned)]
    return low + high


def real_dft(xs):
    n = len(xs)
    if n == 2:
        if xs[1] is None:
            return [(xs[0], None), (xs[0], None)]
        return [(xs[0] + xs[1], None), (xs[0] - xs[1], None)]
    half, quarter = n // 2, n // 4
    total = [a if b is None else a + b for a, b in zip(xs[:half], xs[half:])]
    delta = [a if b is None else a - b for a, b in zip(xs[:half], xs[half:])]
    out = [None] * (half + 1)
    for j, value in enumerate(real_dft(total)):
        out[2 * j] = value
    zs = [
        cmul_const((delta[m], -delta[m + quarter]), root(n, -m)) for m in range(quarter)
    ]
    for j, value in enumerate(complex_dft(zs, -1)):
        k = 4 * j + 1
        if k <= half:
            out[k] = value
        else:
            out[n - k] = (value[0], -value[1])
    return out


def real_inverse(zs):
    n = 2 * (len(zs) - 1)
    if n == 2:
        return [zs[0][0] + zs[1][0], zs[0][0] - zs[1][0]]
    even, odd = real_inverse(zs[0::2]), odd_part(zs)
    return [e + o for e, o in zip(even, odd)] + [e - o for e, o in zip(even, odd)]


def odd_part(zs):
    n = 2 * (len(zs) - 1)
    quarter = n // 4
    picked = []
    for j in range(quarter):
        k = 4 * j + 1
        picked.append(zs[k] if k <= n // 2 else (zs[n - k][0], -zs[n - k][1]))
    turned = [
        cmul_const(z, root(n, m)) for m, z in enumerate(complex_dft(picked, 1))
    ]
    return [2.0 * z[0] for z in turned] + [-2.0 * z[1] for z in turned]


def real_inverse_half(zs):
    return [e + o for e, o in zip(real_inverse(zs[0::2]), odd_part(zs))]


def dft_table(seq_len):
    total = 2 * seq_len
    radix = total // INNER
    k1 = np.arange(radix // 2 + 1)[:, None, None]
    k2 = np.arange(INNER)[None, :, None]
    n2 = np.arange(INNER)[None, None, :]
    angle = 2.0 * np.pi * (n2 * (k1 + radix * k2) % total) / total
    return np.stack([np.cos(angle), np.sin(angle)], axis=1).astype(jnp.bfloat16)


def dot(a, b, dims=((1,), (0,))):
    return lax.dot_general(a, b, (dims, ((), ())), preferred_element_type=f32)


def spectrum(load, table_ref, out_ref, top_ref, bot_ref, saved=None):
    copies = []
    count = out_ref.shape[0]
    lanes = out_ref.shape[2] // 2

    def body(i, carry):
        start = pl.multiple_of(i * ROWS, ROWS)
        rows = pl.ds(start, ROWS)
        blocks = [load(n1, start) for n1 in range(count - 1)]
        for k, (re, im) in enumerate(real_dft(blocks + [None] * (count - 1))):
            re = re.astype(bf16)
            if im is None:
                top_ref[k, rows, :lanes] = re
                bot_ref[k, rows, lanes:] = -re
            else:
                im = im.astype(bf16)
                top_ref[k, rows, :lanes] = re
                top_ref[k, rows, lanes:] = im
                bot_ref[k, rows, :lanes] = im
                bot_ref[k, rows, lanes:] = -re
        return carry

    lax.fori_loop(0, INNER // ROWS, body, 0)
    for k in range(count):
        if k == 0 or k == count - 1:
            out_ref[k, :, :lanes] = dot(table_ref[k, 0], top_ref[k, :, :lanes])
            out_ref[k, :, lanes:] = dot(table_ref[k, 1], bot_ref[k, :, lanes:])
        else:
            out_ref[k] = dot(table_ref[k, 0], top_ref[k]) + dot(table_ref[k, 1], bot_ref[k])
        if saved is not None:
            copies.append(pltpu.make_async_copy(out_ref.at[k], saved[0].at[k], saved[1].at[k]))
            copies[-1].start()
    return copies


def product_inverse(a_ref, b_ref, conj_a, table_ref, z_ref, top_ref, bot_ref, store):
    count = a_ref.shape[0]
    lanes = a_ref.shape[2] // 2
    total = 2 * (count - 1) * INNER
    for k in range(count):
        ar, ai = a_ref[k, :, :lanes], a_ref[k, :, lanes:]
        br, bi = b_ref[k, :, :lanes], b_ref[k, :, lanes:]
        if conj_a:
            re, im = ar * br + ai * bi, ar * bi - ai * br
        else:
            re, im = ar * br - ai * bi, ar * bi + ai * br
        re, im = re.astype(bf16), im.astype(bf16)
        top_ref[k, :, :lanes] = re
        bot_ref[k, :, :lanes] = -im
        if 0 < k < count - 1:
            top_ref[k, :, lanes:] = im
            bot_ref[k, :, lanes:] = re
    turn = ((0,), (0,))
    for k in range(count):
        if k == 0 or k == count - 1:
            z_ref[k, :, :lanes] = dot(table_ref[k, 0], top_ref[k, :, :lanes], turn) + dot(
                table_ref[k, 1], bot_ref[k, :, :lanes], turn
            )
        else:
            z_ref[k] = dot(table_ref[k, 0], top_ref[k], turn) + dot(
                table_ref[k, 1], bot_ref[k], turn
            )

    def body(i, carry):
        start = pl.multiple_of(i * ROWS, ROWS)
        rows = pl.ds(start, ROWS)
        zs = []
        for k in range(count):
            re = z_ref[k, rows, :lanes]
            zs.append((re, None if k in (0, count - 1) else z_ref[k, rows, lanes:]))
        for n1, value in enumerate(real_inverse_half(zs)):
            store(n1, start, value * (1.0 / total))
        return carry

    lax.fori_loop(0, INNER // ROWS, body, 0)


def filter_kernel(filters_ref, table_ref, saved_ref, spec_ref, turned_ref, top_ref, bot_ref, sems):
    count = spec_ref.shape[0]
    for n1 in range(count - 1):
        turned_ref[n1] = filters_ref[:, n1 * INNER : (n1 + 1) * INNER].T
    for copy in spectrum(
        lambda n1, start: turned_ref[n1, pl.ds(start, ROWS)],
        table_ref,
        spec_ref,
        top_ref,
        bot_ref,
        (saved_ref, sems),
    ):
        copy.wait()


def conv_kernel(
    mixed_ref,
    filters_ref,
    table_ref,
    conv_ref,
    saved_ref,
    filt_ref,
    spec_ref,
    z_ref,
    top_ref,
    bot_ref,
    sems,
    sem,
):
    fetch = pltpu.make_async_copy(filters_ref, filt_ref, sem)
    fetch.start()
    copies = spectrum(
        lambda n1, start: mixed_ref[pl.ds(n1 * INNER + start, ROWS)].astype(f32),
        table_ref,
        spec_ref,
        top_ref,
        bot_ref,
        (saved_ref, sems),
    )
    fetch.wait()

    def store(n1, start, value):
        conv_ref[pl.ds(n1 * INNER + start, ROWS)] = value.astype(bf16)

    product_inverse(filt_ref, spec_ref, False, table_ref, z_ref, top_ref, bot_ref, store)
    for copy in copies:
        copy.wait()


def grad_kernel(n_chunks, *refs):
    chunk_refs, (weight_ref, out_ref, rows_ref) = refs[:n_chunks], refs[n_chunks:]
    rows = chunk_refs[0].shape[0]
    for i, ref in enumerate(chunk_refs):
        rows_ref[i * rows : (i + 1) * rows] = ref[...]
    out_ref[...] = dot(rows_ref[...], weight_ref[...], ((1,), (1,))).astype(bf16)


def split_kernel(key_ref, value_ref, query_ref, mixed_ref, out_ref):
    n, _, chan = out_ref.shape
    for p in range(n):
        cols = slice(p * chan, (p + 1) * chan)
        mixed = key_ref[:, cols].astype(f32) * value_ref[:, cols].astype(f32)
        mixed_ref[p] = mixed.astype(bf16)
        out_ref[p] = query_ref[:, cols]


def finish_kernel(got_ref, key_ref, value_ref, grad_query_ref, grad_key_ref, grad_value_ref):
    n, _, _, chan = got_ref.shape
    for p in range(n):
        cols = slice(p * chan, (p + 1) * chan)
        grad_query_ref[:, cols] = got_ref[p, 0]
        back = got_ref[p, 1].astype(f32)
        grad_key_ref[:, cols] = (back * value_ref[:, cols].astype(f32)).astype(bf16)
        grad_value_ref[:, cols] = (back * key_ref[:, cols].astype(f32)).astype(bf16)


def tail_kernel(n_parts, n_chunks, where_ref, *refs):
    part_refs, refs = refs[:n_parts], refs[n_parts:]
    chunk_refs, refs = refs[:n_chunks], refs[n_chunks:]
    weight_ref, query_ref, conv_ref, filters_ref, table_ref, *refs = refs
    out_ref, saved_ref, scaled_ref, rows_ref, grad_ref, *refs = refs
    filt_ref, spec_ref, z_ref, top_ref, bot_ref, sems, sem = refs
    fetch = pltpu.make_async_copy(filters_ref, filt_ref, sem)
    fetch.start()
    rows = chunk_refs[0].shape[0]
    _, _, local_t, _ = out_ref.shape
    halves = local_t // rows
    weight = weight_ref[...]
    i = 0

    def scale(grad, unit):
        block, start = unit // halves, pl.multiple_of(unit % halves * rows, rows)
        here, place = pl.ds(start, rows), pl.ds(pl.multiple_of(unit * rows, rows), rows)
        query = query_ref[place].astype(f32)
        scaled_ref[place] = (grad * query).astype(bf16)
        out_ref[block, 0, here] = (grad * conv_ref[place].astype(f32)).astype(bf16)

    for ref in part_refs:
        for j in range(ref.shape[0] // rows):
            scale(ref[j * rows : (j + 1) * rows].astype(f32), where_ref[i])
            i += 1
    for j, ref in enumerate(chunk_refs):
        rows_ref[j * rows : (j + 1) * rows] = ref[...]
    grad_ref[...] = dot(rows_ref[...], weight, ((1,), (1,))).astype(bf16)
    for j in range(n_chunks):
        scale(grad_ref[j * rows : (j + 1) * rows].astype(f32), where_ref[i + j])
    copies = spectrum(
        lambda n1, start: scaled_ref[pl.ds(n1 * INNER + start, ROWS)].astype(f32),
        table_ref,
        spec_ref,
        top_ref,
        bot_ref,
        (saved_ref, sems),
    )
    fetch.wait()

    def store(n1, start, value):
        token = n1 * INNER + start
        here = pl.ds(pl.multiple_of(token % local_t, ROWS), ROWS)
        out_ref[token // local_t, 1, here] = value.astype(bf16)

    product_inverse(filt_ref, spec_ref, True, table_ref, z_ref, top_ref, bot_ref, store)
    for copy in copies:
        copy.wait()


def taps_kernel(
    saved_mix, saved_grad, table_ref, out_ref, mix_ref, grad_ref, z_ref, top_ref, bot_ref, turned_ref, sems
):
    fetch = [
        pltpu.make_async_copy(saved_mix, mix_ref, sems.at[0]),
        pltpu.make_async_copy(saved_grad, grad_ref, sems.at[1]),
    ]
    for copy in fetch:
        copy.start()
    for copy in fetch:
        copy.wait()

    def store(n1, start, value):
        turned_ref[n1, pl.ds(start, ROWS)] = value

    product_inverse(mix_ref, grad_ref, True, table_ref, z_ref, top_ref, bot_ref, store)
    for n1 in range(mix_ref.shape[0] - 1):
        out_ref[:, n1 * INNER : (n1 + 1) * INNER] = turned_ref[n1].T.astype(bf16)


def weight_kernel(n_chunks, first, unit, where_ref, *refs):
    chunk_refs, rest = refs[:n_chunks], refs[n_chunks:]
    query_ref, conv_ref, *rest = rest
    if not first:
        sum_ref, rest = rest[0], rest[1:]
    (out_ref,) = rest
    gated, i = [], 0
    for ref in chunk_refs:
        for _ in range(ref.shape[0] // unit):
            place = pl.ds(pl.multiple_of(where_ref[i] * unit, unit), unit)
            wide = query_ref[place].astype(f32) * conv_ref[place].astype(f32)
            gated.append(wide.astype(bf16))
            i += 1
    left = jnp.concatenate(gated, axis=0)
    width = chunk_refs[0].shape[1]
    step = 512 if width % 512 == 0 else width
    for c in range(0, width, step):
        right = jnp.concatenate([r[:, c : c + step] for r in chunk_refs], axis=0)
        acc = dot(left, right, ((0,), (0,)))
        if not first:
            acc = acc + sum_ref[:, c : c + step]
        out_ref[:, c : c + step] = acc.astype(out_ref.dtype)


def vmem():
    return pl.BlockSpec(memory_space=pltpu.VMEM)


def hbm():
    return pl.BlockSpec(memory_space=pltpu.HBM)


def smem():
    return pl.BlockSpec(memory_space=pltpu.SMEM)


def in_hbm(x):
    return pltpu.with_memory_space_constraint(x, pltpu.HBM)


def call(kernel, outs, n_in, scratch=(), scalars=0, flops=0, kept=(), saved=None):
    ins = [hbm() if i in kept else vmem() for i in range(n_in)]
    many = isinstance(outs, tuple)
    specs = [hbm() if i == saved else vmem() for i in range(len(outs) if many else 1)]
    return pl.pallas_call(
        kernel,
        out_shape=outs,
        in_specs=[smem()] * scalars + ins,
        out_specs=tuple(specs) if many else specs[0],
        scratch_shapes=list(scratch),
        compiler_params=pltpu.CompilerParams(vmem_limit_bytes=VMEM_LIMIT),
        cost_estimate=pl.CostEstimate(flops=flops, bytes_accessed=1 << 20, transcendentals=0),
    )


def chip_cycle(chips):
    rows = 1 << (chips.bit_length() // 2)
    while chips % rows:
        rows //= 2
    cols = chips // rows
    if cols == 1 or rows % 2:
        return list(range(chips))
    order = [r * cols for r in range(rows)]
    for i, r in enumerate(reversed(range(rows))):
        across = list(range(1, cols))
        order += [r * cols + c for c in (across if i % 2 == 0 else reversed(across))]
    return order


def per_device(size, queries, keys, values, upstream, filters, out_weight):
    chips = size // 2
    cycle = chip_cycle(chips)
    place = {chip: i for i, chip in enumerate(cycle)}
    forward = []
    for i, chip in enumerate(cycle):
        for core in range(2):
            forward.append((2 * chip + core, 2 * cycle[(i + 1) % chips] + core))
    backward = [(b, a) for a, b in forward]
    partner = [(i, i ^ 1) for i in range(size)]

    def sources(offset, other):
        table = []
        for p in range(size):
            chip = cycle[(place[p // 2] + offset) % chips]
            table.append(2 * chip + ((p % 2) ^ other))
        return table

    rows, queries_rows = upstream[0], queries[0]
    key_rows, value_rows = keys[0], values[0]
    local_t, width = rows.shape
    chan = out_weight.shape[0]
    seq_len = filters.shape[1]
    count = seq_len // INNER + 1
    table = jnp.asarray(dft_table(seq_len))
    spec = pltpu.HBM((count, INNER, 2 * chan), f32)
    chan_bf = pltpu.HBM((seq_len, chan), bf16)
    sem, sems = pltpu.SemaphoreType.DMA(()), pltpu.SemaphoreType.DMA((count,))
    top = pltpu.VMEM((count, INNER, 2 * chan), bf16)
    zs = pltpu.VMEM((count, INNER, 2 * chan), f32)
    turned = pltpu.VMEM((count - 1, INNER, chan), f32)
    one = 8 * count * INNER * INNER * chan

    half = local_t // 2
    steps = chips // 2
    me = lax.axis_index("ctx")

    def to_partner(x):
        return lax.ppermute(x, "ctx", partner)

    def exchange(x):
        return lax.all_to_all(x, "ctx", 0, 0, tiled=True)

    def grad_of(group):
        n = len(group)
        return call(
            functools.partial(grad_kernel, n),
            pltpu.HBM((n * local_t, chan), bf16),
            n + 1,
            [pltpu.VMEM((n * local_t, width), bf16)],
            flops=2 * n * local_t * width * chan,
        )(*[g[0] for g in group], out_weight)

    def pair(x, offset, halves=(0, 1)):
        return [(x, offset, 0, halves), (to_partner(x), offset, 1, halves)]

    blocks = pltpu.HBM((size, 2, local_t, chan), bf16)
    block = pltpu.HBM((size, local_t, chan), bf16)
    mixed, query = call(split_kernel, (block, block), 3, flops=seq_len * chan)(
        in_hbm(key_rows), in_hbm(value_rows), in_hbm(queries_rows)
    )
    mixed = exchange(mixed).reshape(seq_len, chan)
    query = exchange(query).reshape(seq_len, chan)
    filt_spec = call(filter_kernel, spec, 2, [zs, turned, top, top, sems], flops=one, saved=0)(
        in_hbm(filters), table
    )
    groups = [pair(rows, 0)]
    parts = []
    ahead, behind = rows, rows
    for step in range(1, steps):
        ahead = lax.ppermute(ahead, "ctx", forward)
        behind = lax.ppermute(behind, "ctx", backward)
        groups.append(pair(ahead, -step) + pair(behind, step))
        parts.append(grad_of(groups[step - 1]))
    ahead = lax.ppermute(ahead[:half], "ctx", forward)
    behind = lax.ppermute(behind[half:], "ctx", backward)
    parts.append(grad_of(groups[-1]))
    conv_chan, mix_spec = call(
        conv_kernel,
        (chan_bf, spec),
        3,
        [zs, zs, zs, top, top, sems, sem],
        flops=2 * one,
        kept=(1,),
        saved=1,
    )(mixed, in_hbm(filt_spec), table)
    groups.append(pair(ahead, -steps, (0,)) + pair(behind, -steps, (1,)))

    where = [[2 * p + h for p in sources(g[1], g[2])] for group in groups for g in group for h in g[3]]
    where = jnp.asarray(np.array(where, np.int32).T)[me]

    def weight_of(members, total, dtype):
        pieces = [g[0] for i in members for g in groups[i]]
        before = sum(len(g[3]) for i in range(members[0]) for g in groups[i])
        units = sum(len(g[3]) for i in members for g in groups[i])
        first = total is None
        return call(
            functools.partial(weight_kernel, len(pieces), first, half),
            jax.ShapeDtypeStruct((chan, width), dtype),
            len(pieces) + 2 + (not first),
            scalars=1,
            flops=2 * units * half * width * chan,
        )(where[before : before + units], *pieces, query, conv_chan, *(() if first else (total,)))

    total = weight_of(range(steps - 1), None, f32)
    total = weight_of([steps - 1], total, f32)
    part_weight = weight_of([steps], total, bf16)
    final = [g[0] for g in groups[-1]]

    back, grad_spec = call(
        functools.partial(tail_kernel, len(parts), len(final)),
        (blocks, spec),
        len(parts) + len(final) + 5,
        [
            pltpu.VMEM((seq_len, chan), bf16),
            pltpu.VMEM((len(final) * half, width), bf16),
            pltpu.VMEM((len(final) * half, chan), bf16),
            zs,
            zs,
            zs,
            top,
            top,
            sems,
            sem,
        ],
        scalars=1,
        flops=2 * one,
        kept=(len(parts) + len(final) + 3,),
        saved=1,
    )(where, *parts, *final, out_weight, query, conv_chan, in_hbm(filt_spec), table)
    back = exchange(back)

    taps = call(
        taps_kernel,
        jax.ShapeDtypeStruct((chan, seq_len), bf16),
        3,
        [zs, zs, zs, top, top, turned, pltpu.SemaphoreType.DMA((2,))],
        flops=one,
        kept=(0, 1),
    )(in_hbm(mix_spec), in_hbm(grad_spec), table)
    rows_bf = jax.ShapeDtypeStruct((local_t, size * chan), bf16)
    grad_queries, grad_keys, grad_values = call(
        finish_kernel, (rows_bf, rows_bf, rows_bf), 3, flops=seq_len * chan
    )(back, key_rows, value_rows)

    def over_dp(x):
        n = lax.axis_size("dp")
        total = x.astype(f32)
        if n == 2:
            return total + lax.ppermute(x, "dp", [(0, 1), (1, 0)]).astype(f32)
        return lax.psum(x, "dp").astype(f32)

    return (
        grad_queries[None], grad_keys[None], grad_values[None], over_dp(taps), over_dp(part_weight)
    )


def solution(mesh):
    tokens, chans = P("dp", "ctx", None), P("ctx", None)

    def body(*args):
        return per_device(mesh.shape["ctx"], *args)

    return jax.shard_map(
        body,
        mesh=mesh,
        in_specs=(tokens, tokens, tokens, tokens, chans, chans),
        out_specs=(tokens, tokens, tokens, chans, chans),
        check_vma=False,
    )
```

```python
import functools
import math

import jax
import jax.numpy as jnp
import numpy as np
from jax import lax
from jax.experimental import pallas as pl
from jax.experimental.pallas import tpu as pltpu
from jax.sharding import PartitionSpec as P


INNER = 256
ROWS = 32
VMEM_LIMIT = 20 << 20
f32 = jnp.float32
bf16 = jnp.bfloat16


def cmul_const(z, c):
    re, im = z
    if abs(c.imag) < 1e-12:
        return (re, im) if abs(c.real - 1) < 1e-12 else (re * c.real, im * c.real)
    if abs(c.real) < 1e-12:
        if abs(c.imag - 1) < 1e-12:
            return (-im, re)
        if abs(c.imag + 1) < 1e-12:
            return (im, -re)
    return (re * c.real - im * c.imag, re * c.imag + im * c.real)


def root(n, k):
    angle = 2.0 * math.pi * (k % n) / n
    return complex(math.cos(angle), math.sin(angle))


def complex_dft(zs, sign):
    n = len(zs)
    if n == 1:
        return zs
    even = complex_dft(zs[0::2], sign)
    odd = complex_dft(zs[1::2], sign)
    turned = [cmul_const(odd[k], root(n, sign * k)) for k in range(n // 2)]
    low = [(e[0] + t[0], e[1] + t[1]) for e, t in zip(even, turned)]
    high = [(e[0] - t[0], e[1] - t[1]) for e, t in zip(even, turned)]
    return low + high


def real_dft(xs):
    n = len(xs)
    if n == 2:
        if xs[1] is None:
            return [(xs[0], None), (xs[0], None)]
        return [(xs[0] + xs[1], None), (xs[0] - xs[1], None)]
    half, quarter = n // 2, n // 4
    total = [a if b is None else a + b for a, b in zip(xs[:half], xs[half:])]
    delta = [a if b is None else a - b for a, b in zip(xs[:half], xs[half:])]
    out = [None] * (half + 1)
    for j, value in enumerate(real_dft(total)):
        out[2 * j] = value
    zs = [
        cmul_const((delta[m], -delta[m + quarter]), root(n, -m)) for m in range(quarter)
    ]
    for j, value in enumerate(complex_dft(zs, -1)):
        k = 4 * j + 1
        if k <= half:
            out[k] = value
        else:
            out[n - k] = (value[0], -value[1])
    return out


def real_inverse(zs):
    n = 2 * (len(zs) - 1)
    if n == 2:
        return [zs[0][0] + zs[1][0], zs[0][0] - zs[1][0]]
    even, odd = real_inverse(zs[0::2]), odd_part(zs)
    return [e + o for e, o in zip(even, odd)] + [e - o for e, o in zip(even, odd)]


def odd_part(zs):
    n = 2 * (len(zs) - 1)
    quarter = n // 4
    picked = []
    for j in range(quarter):
        k = 4 * j + 1
        picked.append(zs[k] if k <= n // 2 else (zs[n - k][0], -zs[n - k][1]))
    turned = [
        cmul_const(z, root(n, m)) for m, z in enumerate(complex_dft(picked, 1))
    ]
    return [2.0 * z[0] for z in turned] + [-2.0 * z[1] for z in turned]


def real_inverse_half(zs):
    return [e + o for e, o in zip(real_inverse(zs[0::2]), odd_part(zs))]


def dft_table(seq_len):
    total = 2 * seq_len
    radix = total // INNER
    k1 = np.arange(radix // 2 + 1)[:, None, None]
    k2 = np.arange(INNER)[None, :, None]
    n2 = np.arange(INNER)[None, None, :]
    angle = 2.0 * np.pi * (n2 * (k1 + radix * k2) % total) / total
    return np.stack([np.cos(angle), np.sin(angle)], axis=1).astype(jnp.bfloat16)


def dot(a, b, dims=((1,), (0,))):
    return lax.dot_general(a, b, (dims, ((), ())), preferred_element_type=f32)


def spectrum(load, table_ref, out_ref, top_ref, bot_ref, saved=None):
    copies = []
    count = out_ref.shape[0]
    lanes = out_ref.shape[2] // 2

    def body(i, carry):
        start = pl.multiple_of(i * ROWS, ROWS)
        rows = pl.ds(start, ROWS)
        blocks = [load(n1, start) for n1 in range(count - 1)]
        for k, (re, im) in enumerate(real_dft(blocks + [None] * (count - 1))):
            re = re.astype(bf16)
            if im is None:
                top_ref[k, rows, :lanes] = re
                bot_ref[k, rows, lanes:] = -re
            else:
                im = im.astype(bf16)
                top_ref[k, rows, :lanes] = re
                top_ref[k, rows, lanes:] = im
                bot_ref[k, rows, :lanes] = im
                bot_ref[k, rows, lanes:] = -re
        return carry

    lax.fori_loop(0, INNER // ROWS, body, 0)
    for k in range(count):
        if k == 0 or k == count - 1:
            out_ref[k, :, :lanes] = dot(table_ref[k, 0], top_ref[k, :, :lanes])
            out_ref[k, :, lanes:] = dot(table_ref[k, 1], bot_ref[k, :, lanes:])
        else:
            out_ref[k] = dot(table_ref[k, 0], top_ref[k]) + dot(table_ref[k, 1], bot_ref[k])
        if saved is not None:
            copies.append(pltpu.make_async_copy(out_ref.at[k], saved[0].at[k], saved[1].at[k]))
            copies[-1].start()
    return copies


def product_inverse(a_ref, b_ref, conj_a, table_ref, z_ref, top_ref, bot_ref, store):
    count = a_ref.shape[0]
    lanes = a_ref.shape[2] // 2
    total = 2 * (count - 1) * INNER
    for k in range(count):
        ar, ai = a_ref[k, :, :lanes], a_ref[k, :, lanes:]
        br, bi = b_ref[k, :, :lanes], b_ref[k, :, lanes:]
        if conj_a:
            re, im = ar * br + ai * bi, ar * bi - ai * br
        else:
            re, im = ar * br - ai * bi, ar * bi + ai * br
        re, im = re.astype(bf16), im.astype(bf16)
        top_ref[k, :, :lanes] = re
        bot_ref[k, :, :lanes] = -im
        if 0 < k < count - 1:
            top_ref[k, :, lanes:] = im
            bot_ref[k, :, lanes:] = re
    turn = ((0,), (0,))
    for k in range(count):
        if k == 0 or k == count - 1:
            z_ref[k, :, :lanes] = dot(table_ref[k, 0], top_ref[k, :, :lanes], turn) + dot(
                table_ref[k, 1], bot_ref[k, :, :lanes], turn
            )
        else:
            z_ref[k] = dot(table_ref[k, 0], top_ref[k], turn) + dot(
                table_ref[k, 1], bot_ref[k], turn
            )

    def body(i, carry):
        start = pl.multiple_of(i * ROWS, ROWS)
        rows = pl.ds(start, ROWS)
        zs = []
        for k in range(count):
            re = z_ref[k, rows, :lanes]
            zs.append((re, None if k in (0, count - 1) else z_ref[k, rows, lanes:]))
        for n1, value in enumerate(real_inverse_half(zs)):
            store(n1, start, value * (1.0 / total))
        return carry

    lax.fori_loop(0, INNER // ROWS, body, 0)


def filter_kernel(filters_ref, table_ref, saved_ref, spec_ref, turned_ref, top_ref, bot_ref, sems):
    count = spec_ref.shape[0]
    for n1 in range(count - 1):
        turned_ref[n1] = filters_ref[:, n1 * INNER : (n1 + 1) * INNER].T
    for copy in spectrum(
        lambda n1, start: turned_ref[n1, pl.ds(start, ROWS)],
        table_ref,
        spec_ref,
        top_ref,
        bot_ref,
        (saved_ref, sems),
    ):
        copy.wait()


def conv_kernel(
    mixed_ref,
    filters_ref,
    table_ref,
    conv_ref,
    saved_ref,
    filt_ref,
    spec_ref,
    z_ref,
    top_ref,
    bot_ref,
    sems,
    sem,
):
    fetch = pltpu.make_async_copy(filters_ref, filt_ref, sem)
    fetch.start()
    copies = spectrum(
        lambda n1, start: mixed_ref[pl.ds(n1 * INNER + start, ROWS)].astype(f32),
        table_ref,
        spec_ref,
        top_ref,
        bot_ref,
        (saved_ref, sems),
    )
    fetch.wait()

    def store(n1, start, value):
        conv_ref[pl.ds(n1 * INNER + start, ROWS)] = value.astype(bf16)

    product_inverse(filt_ref, spec_ref, False, table_ref, z_ref, top_ref, bot_ref, store)
    for copy in copies:
        copy.wait()


def grad_kernel(n_chunks, *refs):
    chunk_refs, (weight_ref, out_ref, rows_ref) = refs[:n_chunks], refs[n_chunks:]
    rows = chunk_refs[0].shape[0]
    for i, ref in enumerate(chunk_refs):
        rows_ref[i * rows : (i + 1) * rows] = ref[...]
    out_ref[...] = dot(rows_ref[...], weight_ref[...]).astype(bf16)


def turn_kernel(in_ref, out_ref):
    out_ref[...] = in_ref[...].astype(f32).T.astype(bf16)


def mix_kernel(key_ref, value_ref, out_ref):
    n, _, chan = out_ref.shape
    for p in range(n):
        cols = slice(p * chan, (p + 1) * chan)
        mixed = key_ref[:, cols].astype(f32) * value_ref[:, cols].astype(f32)
        out_ref[p] = mixed.astype(bf16)


def split_kernel(in_ref, out_ref):
    n, _, chan = out_ref.shape
    for p in range(n):
        out_ref[p] = in_ref[:, p * chan : (p + 1) * chan]


def cut_kernel(start, in_ref, out_ref):
    out_ref[...] = in_ref[start : start + out_ref.shape[0]]


def finish_kernel(got_ref, key_ref, value_ref, grad_query_ref, grad_key_ref, grad_value_ref):
    n, _, _, chan = got_ref.shape
    for p in range(n):
        cols = slice(p * chan, (p + 1) * chan)
        grad_query_ref[:, cols] = got_ref[p, 0]
        back = got_ref[p, 1].astype(f32)
        grad_key_ref[:, cols] = (back * value_ref[:, cols].astype(f32)).astype(bf16)
        grad_value_ref[:, cols] = (back * key_ref[:, cols].astype(f32)).astype(bf16)


def tail_kernel(n_parts, n_chunks, where_ref, *refs):
    part_refs, refs = refs[:n_parts], refs[n_parts:]
    chunk_refs, refs = refs[:n_chunks], refs[n_chunks:]
    weight_ref, query_ref, conv_ref, filters_ref, table_ref, *refs = refs
    out_ref, saved_ref, scaled_ref, rows_ref, grad_ref, *refs = refs
    filt_ref, spec_ref, z_ref, top_ref, bot_ref, sems, sem = refs
    fetch = pltpu.make_async_copy(filters_ref, filt_ref, sem)
    fetch.start()
    rows = chunk_refs[0].shape[0]
    _, _, local_t, _ = out_ref.shape
    halves = local_t // rows
    weight = weight_ref[...]
    i = 0

    def scale(grad, unit):
        block, start = unit // halves, pl.multiple_of(unit % halves * rows, rows)
        here, place = pl.ds(start, rows), pl.ds(pl.multiple_of(unit * rows, rows), rows)
        query = query_ref[place].astype(f32)
        scaled_ref[place] = (grad * query).astype(bf16)
        out_ref[block, 0, here] = (grad * conv_ref[place].astype(f32)).astype(bf16)

    for ref in part_refs:
        for j in range(ref.shape[0] // rows):
            scale(ref[j * rows : (j + 1) * rows].astype(f32), where_ref[i])
            i += 1
    for j, ref in enumerate(chunk_refs):
        rows_ref[j * rows : (j + 1) * rows] = ref[...]
    grad_ref[...] = dot(rows_ref[...], weight).astype(bf16)
    for j in range(n_chunks):
        scale(grad_ref[j * rows : (j + 1) * rows].astype(f32), where_ref[i + j])
    copies = spectrum(
        lambda n1, start: scaled_ref[pl.ds(n1 * INNER + start, ROWS)].astype(f32),
        table_ref,
        spec_ref,
        top_ref,
        bot_ref,
        (saved_ref, sems),
    )
    fetch.wait()

    def store(n1, start, value):
        token = n1 * INNER + start
        here = pl.ds(pl.multiple_of(token % local_t, ROWS), ROWS)
        out_ref[token // local_t, 1, here] = value.astype(bf16)

    product_inverse(filt_ref, spec_ref, True, table_ref, z_ref, top_ref, bot_ref, store)
    for copy in copies:
        copy.wait()


def taps_kernel(
    saved_mix, saved_grad, table_ref, out_ref, mix_ref, grad_ref, z_ref, top_ref, bot_ref, turned_ref, sems
):
    fetch = [
        pltpu.make_async_copy(saved_mix, mix_ref, sems.at[0]),
        pltpu.make_async_copy(saved_grad, grad_ref, sems.at[1]),
    ]
    for copy in fetch:
        copy.start()
    for copy in fetch:
        copy.wait()

    def store(n1, start, value):
        turned_ref[n1, pl.ds(start, ROWS)] = value

    product_inverse(mix_ref, grad_ref, True, table_ref, z_ref, top_ref, bot_ref, store)
    for n1 in range(mix_ref.shape[0] - 1):
        out_ref[:, n1 * INNER : (n1 + 1) * INNER] = turned_ref[n1].T.astype(bf16)


def weight_kernel(n_chunks, first, unit, where_ref, *refs):
    chunk_refs, rest = refs[:n_chunks], refs[n_chunks:]
    query_ref, conv_ref, *rest = rest
    if not first:
        sum_ref, rest = rest[0], rest[1:]
    (out_ref,) = rest
    gated, i = [], 0
    for ref in chunk_refs:
        for _ in range(ref.shape[0] // unit):
            place = pl.ds(pl.multiple_of(where_ref[i] * unit, unit), unit)
            wide = query_ref[place].astype(f32) * conv_ref[place].astype(f32)
            gated.append(wide.astype(bf16))
            i += 1
    left = jnp.concatenate(gated, axis=0)
    width = chunk_refs[0].shape[1]
    step = 512 if width % 512 == 0 else width
    for c in range(0, width, step):
        right = jnp.concatenate([r[:, c : c + step] for r in chunk_refs], axis=0)
        acc = dot(left, right, ((0,), (0,)))
        if not first:
            acc = acc + sum_ref[:, c : c + step]
        out_ref[:, c : c + step] = acc.astype(out_ref.dtype)


def vmem():
    return pl.BlockSpec(memory_space=pltpu.VMEM)


def hbm():
    return pl.BlockSpec(memory_space=pltpu.HBM)


def smem():
    return pl.BlockSpec(memory_space=pltpu.SMEM)


def in_hbm(x):
    return pltpu.with_memory_space_constraint(x, pltpu.HBM)


def call(kernel, outs, n_in, scratch=(), scalars=0, flops=0, kept=(), saved=None):
    ins = [hbm() if i in kept else vmem() for i in range(n_in)]
    many = isinstance(outs, tuple)
    specs = [hbm() if i == saved else vmem() for i in range(len(outs) if many else 1)]
    return pl.pallas_call(
        kernel,
        out_shape=outs,
        in_specs=[smem()] * scalars + ins,
        out_specs=tuple(specs) if many else specs[0],
        scratch_shapes=list(scratch),
        compiler_params=pltpu.CompilerParams(vmem_limit_bytes=VMEM_LIMIT),
        cost_estimate=pl.CostEstimate(flops=flops, bytes_accessed=1 << 20, transcendentals=0),
    )


def chip_cycle(chips):
    rows = 1 << (chips.bit_length() // 2)
    while chips % rows:
        rows //= 2
    cols = chips // rows
    if cols == 1 or rows % 2:
        return list(range(chips))
    order = [r * cols for r in range(rows)]
    for i, r in enumerate(reversed(range(rows))):
        across = list(range(1, cols))
        order += [r * cols + c for c in (across if i % 2 == 0 else reversed(across))]
    return order


def per_device(size, queries, keys, values, upstream, filters, out_weight):
    chips = size // 2
    cycle = chip_cycle(chips)
    place = {chip: i for i, chip in enumerate(cycle)}
    forward = []
    for i, chip in enumerate(cycle):
        for core in range(2):
            forward.append((2 * chip + core, 2 * cycle[(i + 1) % chips] + core))
    backward = [(b, a) for a, b in forward]
    partner = [(i, i ^ 1) for i in range(size)]

    def sources(offset, other):
        table = []
        for p in range(size):
            chip = cycle[(place[p // 2] + offset) % chips]
            table.append(2 * chip + ((p % 2) ^ other))
        return table

    rows, queries_rows = upstream[0], queries[0]
    key_rows, value_rows = keys[0], values[0]
    local_t, width = rows.shape
    chan = out_weight.shape[0]
    seq_len = filters.shape[1]
    count = seq_len // INNER + 1
    table = jnp.asarray(dft_table(seq_len))
    spec = pltpu.HBM((count, INNER, 2 * chan), f32)
    chan_bf = pltpu.HBM((seq_len, chan), bf16)
    sem, sems = pltpu.SemaphoreType.DMA(()), pltpu.SemaphoreType.DMA((count,))
    top = pltpu.VMEM((count, INNER, 2 * chan), bf16)
    zs = pltpu.VMEM((count, INNER, 2 * chan), f32)
    turned = pltpu.VMEM((count - 1, INNER, chan), f32)
    one = 8 * count * INNER * INNER * chan

    half = local_t // 2
    steps = chips // 2
    me = lax.axis_index("ctx")

    def to_partner(x):
        return lax.ppermute(x, "ctx", partner)

    def cut(x, start):
        out = jax.ShapeDtypeStruct((half, width), bf16)
        return call(functools.partial(cut_kernel, start), out, 1, flops=half * width)(x)

    def exchange(x):
        return lax.all_to_all(x, "ctx", 0, 0, tiled=True)

    def grad_of(group):
        n = len(group)
        return call(
            functools.partial(grad_kernel, n),
            pltpu.HBM((n * local_t, chan), bf16),
            n + 1,
            [pltpu.VMEM((n * local_t, width), bf16)],
            flops=2 * n * local_t * width * chan,
        )(*[g[0] for g in group], turned_weight)

    def pair(x, offset, halves=(0, 1)):
        return [(x, offset, 0, halves), (to_partner(x), offset, 1, halves)]

    turned_weight = call(
        turn_kernel, jax.ShapeDtypeStruct((width, chan), bf16), 1, flops=width * chan
    )(out_weight)
    blocks = pltpu.HBM((size, 2, local_t, chan), bf16)
    block = pltpu.HBM((size, local_t, chan), bf16)
    mixed = call(mix_kernel, block, 2, flops=seq_len * chan)(in_hbm(key_rows), in_hbm(value_rows))
    query = call(split_kernel, block, 1, flops=seq_len * chan)(in_hbm(queries_rows))
    mixed = exchange(mixed).reshape(seq_len, chan)
    query = exchange(query).reshape(seq_len, chan)
    filt_spec = call(filter_kernel, spec, 2, [zs, turned, top, top, sems], flops=one, saved=0)(
        in_hbm(filters), table
    )
    groups = [pair(rows, 0)]
    parts = []
    ahead, behind = rows, rows
    for step in range(1, steps):
        ahead = lax.ppermute(ahead, "ctx", forward)
        behind = lax.ppermute(behind, "ctx", backward)
        groups.append(pair(ahead, -step) + pair(behind, step))
        parts.append(grad_of(groups[step - 1]))
    ahead = lax.ppermute(cut(ahead, 0), "ctx", forward)
    behind = lax.ppermute(cut(behind, half), "ctx", backward)
    parts.append(grad_of(groups[-1]))
    conv_chan, mix_spec = call(
        conv_kernel,
        (chan_bf, spec),
        3,
        [zs, zs, zs, top, top, sems, sem],
        flops=2 * one,
        kept=(1,),
        saved=1,
    )(mixed, in_hbm(filt_spec), table)
    groups.append(pair(ahead, -steps, (0,)) + pair(behind, -steps, (1,)))

    where = [[2 * p + h for p in sources(g[1], g[2])] for group in groups for g in group for h in g[3]]
    where = jnp.asarray(np.array(where, np.int32).T)[me]

    def weight_of(members, total, dtype):
        pieces = [g[0] for i in members for g in groups[i]]
        before = sum(len(g[3]) for i in range(members[0]) for g in groups[i])
        units = sum(len(g[3]) for i in members for g in groups[i])
        first = total is None
        return call(
            functools.partial(weight_kernel, len(pieces), first, half),
            jax.ShapeDtypeStruct((chan, width), dtype),
            len(pieces) + 2 + (not first),
            scalars=1,
            flops=2 * units * half * width * chan,
        )(where[before : before + units], *pieces, query, conv_chan, *(() if first else (total,)))

    total = weight_of(range(steps - 1), None, f32)
    total = weight_of([steps - 1], total, f32)
    part_weight = weight_of([steps], total, bf16)
    final = [g[0] for g in groups[-1]]

    back, grad_spec = call(
        functools.partial(tail_kernel, len(parts), len(final)),
        (blocks, spec),
        len(parts) + len(final) + 5,
        [
            pltpu.VMEM((seq_len, chan), bf16),
            pltpu.VMEM((len(final) * half, width), bf16),
            pltpu.VMEM((len(final) * half, chan), bf16),
            zs,
            zs,
            zs,
            top,
            top,
            sems,
            sem,
        ],
        scalars=1,
        flops=2 * one,
        kept=(len(parts) + len(final) + 3,),
        saved=1,
    )(where, *parts, *final, turned_weight, query, conv_chan, in_hbm(filt_spec), table)
    back = exchange(back)

    taps = call(
        taps_kernel,
        jax.ShapeDtypeStruct((chan, seq_len), bf16),
        3,
        [zs, zs, zs, top, top, turned, pltpu.SemaphoreType.DMA((2,))],
        flops=one,
        kept=(0, 1),
    )(in_hbm(mix_spec), in_hbm(grad_spec), table)
    rows_bf = jax.ShapeDtypeStruct((local_t, size * chan), bf16)
    grad_queries, grad_keys, grad_values = call(
        finish_kernel, (rows_bf, rows_bf, rows_bf), 3, flops=seq_len * chan
    )(back, key_rows, value_rows)

    def over_dp(x):
        n = lax.axis_size("dp")
        total = x.astype(f32)
        if n == 2:
            return total + lax.ppermute(x, "dp", [(0, 1), (1, 0)]).astype(f32)
        return lax.psum(x, "dp").astype(f32)

    return (
        grad_queries[None], grad_keys[None], grad_values[None], over_dp(taps), over_dp(part_weight)
    )


def solution(mesh):
    tokens, chans = P("dp", "ctx", None), P("ctx", None)

    def body(*args):
        return per_device(mesh.shape["ctx"], *args)

    return jax.shard_map(
        body,
        mesh=mesh,
        in_specs=(tokens, tokens, tokens, tokens, chans, chans),
        out_specs=(tokens, tokens, tokens, chans, chans),
        check_vma=False,
    )
```

```python
import functools
import math

import jax
import jax.numpy as jnp
import numpy as np
from jax import lax
from jax.experimental import pallas as pl
from jax.experimental.pallas import tpu as pltpu
from jax.sharding import PartitionSpec as P


INNER = 256
ROWS = 32
VMEM_LIMIT = 20 << 20
f32 = jnp.float32
bf16 = jnp.bfloat16


def cmul_const(z, c):
    re, im = z
    if abs(c.imag) < 1e-12:
        return (re, im) if abs(c.real - 1) < 1e-12 else (re * c.real, im * c.real)
    if abs(c.real) < 1e-12:
        if abs(c.imag - 1) < 1e-12:
            return (-im, re)
        if abs(c.imag + 1) < 1e-12:
            return (im, -re)
    return (re * c.real - im * c.imag, re * c.imag + im * c.real)


def root(n, k):
    angle = 2.0 * math.pi * (k % n) / n
    return complex(math.cos(angle), math.sin(angle))


def complex_dft(zs, sign):
    n = len(zs)
    if n == 1:
        return zs
    even = complex_dft(zs[0::2], sign)
    odd = complex_dft(zs[1::2], sign)
    turned = [cmul_const(odd[k], root(n, sign * k)) for k in range(n // 2)]
    low = [(e[0] + t[0], e[1] + t[1]) for e, t in zip(even, turned)]
    high = [(e[0] - t[0], e[1] - t[1]) for e, t in zip(even, turned)]
    return low + high


def real_dft(xs):
    n = len(xs)
    if n == 2:
        if xs[1] is None:
            return [(xs[0], None), (xs[0], None)]
        return [(xs[0] + xs[1], None), (xs[0] - xs[1], None)]
    half, quarter = n // 2, n // 4
    total = [a if b is None else a + b for a, b in zip(xs[:half], xs[half:])]
    delta = [a if b is None else a - b for a, b in zip(xs[:half], xs[half:])]
    out = [None] * (half + 1)
    for j, value in enumerate(real_dft(total)):
        out[2 * j] = value
    zs = [
        cmul_const((delta[m], -delta[m + quarter]), root(n, -m)) for m in range(quarter)
    ]
    for j, value in enumerate(complex_dft(zs, -1)):
        k = 4 * j + 1
        if k <= half:
            out[k] = value
        else:
            out[n - k] = (value[0], -value[1])
    return out


def real_inverse(zs):
    n = 2 * (len(zs) - 1)
    if n == 2:
        return [zs[0][0] + zs[1][0], zs[0][0] - zs[1][0]]
    even, odd = real_inverse(zs[0::2]), odd_part(zs)
    return [e + o for e, o in zip(even, odd)] + [e - o for e, o in zip(even, odd)]


def odd_part(zs):
    n = 2 * (len(zs) - 1)
    quarter = n // 4
    picked = []
    for j in range(quarter):
        k = 4 * j + 1
        picked.append(zs[k] if k <= n // 2 else (zs[n - k][0], -zs[n - k][1]))
    turned = [
        cmul_const(z, root(n, m)) for m, z in enumerate(complex_dft(picked, 1))
    ]
    return [2.0 * z[0] for z in turned] + [-2.0 * z[1] for z in turned]


def real_inverse_half(zs):
    return [e + o for e, o in zip(real_inverse(zs[0::2]), odd_part(zs))]


def dft_table(seq_len):
    total = 2 * seq_len
    radix = total // INNER
    k1 = np.arange(radix // 2 + 1)[:, None, None]
    k2 = np.arange(INNER)[None, :, None]
    n2 = np.arange(INNER)[None, None, :]
    angle = 2.0 * np.pi * (n2 * (k1 + radix * k2) % total) / total
    return np.stack([np.cos(angle), np.sin(angle)], axis=1).astype(jnp.bfloat16)


def dot(a, b, dims=((1,), (0,))):
    return lax.dot_general(a, b, (dims, ((), ())), preferred_element_type=f32)


def spectrum(load, table_ref, out_ref, pair_ref, saved=None):
    copies = []
    count = out_ref.shape[0]
    lanes = out_ref.shape[2] // 2

    def body(i, carry):
        start = pl.multiple_of(i * ROWS, ROWS)
        rows = pl.ds(start, ROWS)
        blocks = [load(n1, start) for n1 in range(count - 1)]
        for k, (re, im) in enumerate(real_dft(blocks + [None] * (count - 1))):
            pair_ref[k, rows, :lanes] = re.astype(bf16)
            if im is not None:
                pair_ref[k, rows, lanes:] = im.astype(bf16)
        return carry

    lax.fori_loop(0, INNER // ROWS, body, 0)
    for k in range(count):
        if k == 0 or k == count - 1:
            out_ref[k, :, :lanes] = dot(table_ref[k, 0], pair_ref[k, :, :lanes])
            out_ref[k, :, lanes:] = -dot(table_ref[k, 1], pair_ref[k, :, :lanes])
        else:
            cos, sin = dot(table_ref[k, 0], pair_ref[k]), dot(table_ref[k, 1], pair_ref[k])
            out_ref[k, :, :lanes] = cos[:, :lanes] + sin[:, lanes:]
            out_ref[k, :, lanes:] = cos[:, lanes:] - sin[:, :lanes]
        if saved is not None:
            copies.append(pltpu.make_async_copy(out_ref.at[k], saved[0].at[k], saved[1].at[k]))
            copies[-1].start()
    return copies


def product_inverse(a_ref, b_ref, conj_a, table_ref, z_ref, pair_ref, store):
    count = a_ref.shape[0]
    lanes = a_ref.shape[2] // 2
    total = 2 * (count - 1) * INNER
    for k in range(count):
        ar, ai = a_ref[k, :, :lanes], a_ref[k, :, lanes:]
        br, bi = b_ref[k, :, :lanes], b_ref[k, :, lanes:]
        if conj_a:
            re, im = ar * br + ai * bi, ar * bi - ai * br
        else:
            re, im = ar * br - ai * bi, ar * bi + ai * br
        pair_ref[k, :, :lanes] = re.astype(bf16)
        pair_ref[k, :, lanes:] = im.astype(bf16)
    turn = ((0,), (0,))
    for k in range(count):
        if k == 0 or k == count - 1:
            z_ref[k, :, :lanes] = dot(table_ref[k, 0], pair_ref[k, :, :lanes], turn) - dot(
                table_ref[k, 1], pair_ref[k, :, lanes:], turn
            )
        else:
            cos = dot(table_ref[k, 0], pair_ref[k], turn)
            sin = dot(table_ref[k, 1], pair_ref[k], turn)
            z_ref[k, :, :lanes] = cos[:, :lanes] - sin[:, lanes:]
            z_ref[k, :, lanes:] = cos[:, lanes:] + sin[:, :lanes]

    def body(i, carry):
        start = pl.multiple_of(i * ROWS, ROWS)
        rows = pl.ds(start, ROWS)
        zs = []
        for k in range(count):
            re = z_ref[k, rows, :lanes]
            zs.append((re, None if k in (0, count - 1) else z_ref[k, rows, lanes:]))
        for n1, value in enumerate(real_inverse_half(zs)):
            store(n1, start, value * (1.0 / total))
        return carry

    lax.fori_loop(0, INNER // ROWS, body, 0)


def filter_kernel(filters_ref, table_ref, saved_ref, spec_ref, turned_ref, pair_ref, sems):
    count = spec_ref.shape[0]
    for n1 in range(count - 1):
        turned_ref[n1] = filters_ref[:, n1 * INNER : (n1 + 1) * INNER].T
    for copy in spectrum(
        lambda n1, start: turned_ref[n1, pl.ds(start, ROWS)],
        table_ref,
        spec_ref,
        pair_ref,
        (saved_ref, sems),
    ):
        copy.wait()


def conv_kernel(
    mixed_ref,
    filters_ref,
    table_ref,
    conv_ref,
    saved_ref,
    filt_ref,
    spec_ref,
    z_ref,
    pair_ref,
    sems,
    sem,
):
    fetch = pltpu.make_async_copy(filters_ref, filt_ref, sem)
    fetch.start()
    copies = spectrum(
        lambda n1, start: mixed_ref[pl.ds(n1 * INNER + start, ROWS)].astype(f32),
        table_ref,
        spec_ref,
        pair_ref,
        (saved_ref, sems),
    )
    fetch.wait()

    def store(n1, start, value):
        conv_ref[pl.ds(n1 * INNER + start, ROWS)] = value.astype(bf16)

    product_inverse(filt_ref, spec_ref, False, table_ref, z_ref, pair_ref, store)
    for copy in copies:
        copy.wait()


def grad_kernel(n_chunks, *refs):
    chunk_refs, (weight_ref, out_ref) = refs[:n_chunks], refs[n_chunks:]
    row = 0
    for ref in chunk_refs:
        out_ref[row : row + ref.shape[0]] = dot(ref[...], weight_ref[...]).astype(bf16)
        row += ref.shape[0]


def turn_kernel(in_ref, out_ref):
    out_ref[...] = in_ref[...].astype(f32).T.astype(bf16)


def mix_kernel(key_ref, value_ref, out_ref):
    n, _, chan = out_ref.shape
    for p in range(n):
        cols = slice(p * chan, (p + 1) * chan)
        mixed = key_ref[:, cols].astype(f32) * value_ref[:, cols].astype(f32)
        out_ref[p] = mixed.astype(bf16)


def split_kernel(in_ref, out_ref):
    n, _, chan = out_ref.shape
    for p in range(n):
        out_ref[p] = in_ref[:, p * chan : (p + 1) * chan]


def cut_kernel(start, in_ref, out_ref):
    out_ref[...] = in_ref[start : start + out_ref.shape[0]]


def finish_kernel(got_ref, key_ref, value_ref, grad_query_ref, grad_key_ref, grad_value_ref):
    n, _, _, chan = got_ref.shape
    for p in range(n):
        cols = slice(p * chan, (p + 1) * chan)
        grad_query_ref[:, cols] = got_ref[p, 0]
        back = got_ref[p, 1].astype(f32)
        grad_key_ref[:, cols] = (back * value_ref[:, cols].astype(f32)).astype(bf16)
        grad_value_ref[:, cols] = (back * key_ref[:, cols].astype(f32)).astype(bf16)


def tail_kernel(n_parts, n_chunks, where_ref, *refs):
    part_refs, refs = refs[:n_parts], refs[n_parts:]
    chunk_refs, refs = refs[:n_chunks], refs[n_chunks:]
    weight_ref, query_ref, conv_ref, filters_ref, table_ref, *refs = refs
    out_ref, saved_ref, scaled_ref, rows_ref, grad_ref, *refs = refs
    filt_ref, spec_ref, z_ref, pair_ref, sems, sem = refs
    fetch = pltpu.make_async_copy(filters_ref, filt_ref, sem)
    fetch.start()
    rows = chunk_refs[0].shape[0]
    _, _, local_t, _ = out_ref.shape
    halves = local_t // rows
    weight = weight_ref[...]
    i = 0

    def scale(grad, unit):
        block, start = unit // halves, pl.multiple_of(unit % halves * rows, rows)
        here, place = pl.ds(start, rows), pl.ds(pl.multiple_of(unit * rows, rows), rows)
        query = query_ref[place].astype(f32)
        scaled_ref[place] = (grad * query).astype(bf16)
        out_ref[block, 0, here] = (grad * conv_ref[place].astype(f32)).astype(bf16)

    for ref in part_refs:
        for j in range(ref.shape[0] // rows):
            scale(ref[j * rows : (j + 1) * rows].astype(f32), where_ref[i])
            i += 1
    for j, ref in enumerate(chunk_refs):
        rows_ref[j * rows : (j + 1) * rows] = ref[...]
    grad_ref[...] = dot(rows_ref[...], weight).astype(bf16)
    for j in range(n_chunks):
        scale(grad_ref[j * rows : (j + 1) * rows].astype(f32), where_ref[i + j])
    copies = spectrum(
        lambda n1, start: scaled_ref[pl.ds(n1 * INNER + start, ROWS)].astype(f32),
        table_ref,
        spec_ref,
        pair_ref,
        (saved_ref, sems),
    )
    fetch.wait()

    def store(n1, start, value):
        token = n1 * INNER + start
        here = pl.ds(pl.multiple_of(token % local_t, ROWS), ROWS)
        out_ref[token // local_t, 1, here] = value.astype(bf16)

    product_inverse(filt_ref, spec_ref, True, table_ref, z_ref, pair_ref, store)
    for copy in copies:
        copy.wait()


def taps_kernel(
    saved_mix, saved_grad, table_ref, out_ref, mix_ref, grad_ref, z_ref, pair_ref, turned_ref, sems
):
    fetch = [
        pltpu.make_async_copy(saved_mix, mix_ref, sems.at[0]),
        pltpu.make_async_copy(saved_grad, grad_ref, sems.at[1]),
    ]
    for copy in fetch:
        copy.start()
    for copy in fetch:
        copy.wait()

    def store(n1, start, value):
        turned_ref[n1, pl.ds(start, ROWS)] = value

    product_inverse(mix_ref, grad_ref, True, table_ref, z_ref, pair_ref, store)
    for n1 in range(mix_ref.shape[0] - 1):
        out_ref[:, n1 * INNER : (n1 + 1) * INNER] = turned_ref[n1].T.astype(bf16)


def weight_kernel(n_chunks, first, unit, where_ref, *refs):
    chunk_refs, rest = refs[:n_chunks], refs[n_chunks:]
    query_ref, conv_ref, *rest = rest
    if not first:
        sum_ref, rest = rest[0], rest[1:]
    (out_ref,) = rest
    gated, i = [], 0
    for ref in chunk_refs:
        for _ in range(ref.shape[0] // unit):
            place = pl.ds(pl.multiple_of(where_ref[i] * unit, unit), unit)
            wide = query_ref[place].astype(f32) * conv_ref[place].astype(f32)
            gated.append(wide.astype(bf16))
            i += 1
    left = jnp.concatenate(gated, axis=0)
    width = chunk_refs[0].shape[1]
    step = 512 if width % 512 == 0 else width
    for c in range(0, width, step):
        right = jnp.concatenate([r[:, c : c + step] for r in chunk_refs], axis=0)
        acc = dot(left, right, ((0,), (0,)))
        if not first:
            acc = acc + sum_ref[:, c : c + step]
        out_ref[:, c : c + step] = acc.astype(out_ref.dtype)


def vmem():
    return pl.BlockSpec(memory_space=pltpu.VMEM)


def hbm():
    return pl.BlockSpec(memory_space=pltpu.HBM)


def smem():
    return pl.BlockSpec(memory_space=pltpu.SMEM)


def in_hbm(x):
    return pltpu.with_memory_space_constraint(x, pltpu.HBM)


def call(kernel, outs, n_in, scratch=(), scalars=0, flops=0, kept=(), saved=None):
    ins = [hbm() if i in kept else vmem() for i in range(n_in)]
    many = isinstance(outs, tuple)
    specs = [hbm() if i == saved else vmem() for i in range(len(outs) if many else 1)]
    return pl.pallas_call(
        kernel,
        out_shape=outs,
        in_specs=[smem()] * scalars + ins,
        out_specs=tuple(specs) if many else specs[0],
        scratch_shapes=list(scratch),
        compiler_params=pltpu.CompilerParams(vmem_limit_bytes=VMEM_LIMIT),
        cost_estimate=pl.CostEstimate(flops=flops, bytes_accessed=1 << 20, transcendentals=0),
    )


def chip_cycle(chips):
    rows = 1 << (chips.bit_length() // 2)
    while chips % rows:
        rows //= 2
    cols = chips // rows
    if cols == 1 or rows % 2:
        return list(range(chips))
    order = [r * cols for r in range(rows)]
    for i, r in enumerate(reversed(range(rows))):
        across = list(range(1, cols))
        order += [r * cols + c for c in (across if i % 2 == 0 else reversed(across))]
    return order


def per_device(size, queries, keys, values, upstream, filters, out_weight):
    chips = size // 2
    cycle = chip_cycle(chips)
    place = {chip: i for i, chip in enumerate(cycle)}
    forward = []
    for i, chip in enumerate(cycle):
        for core in range(2):
            forward.append((2 * chip + core, 2 * cycle[(i + 1) % chips] + core))
    backward = [(b, a) for a, b in forward]
    partner = [(i, i ^ 1) for i in range(size)]

    def sources(offset, other):
        table = []
        for p in range(size):
            chip = cycle[(place[p // 2] + offset) % chips]
            table.append(2 * chip + ((p % 2) ^ other))
        return table

    rows, queries_rows = upstream[0], queries[0]
    key_rows, value_rows = keys[0], values[0]
    local_t, width = rows.shape
    chan = out_weight.shape[0]
    seq_len = filters.shape[1]
    count = seq_len // INNER + 1
    table = jnp.asarray(dft_table(seq_len))
    spec = pltpu.HBM((count, INNER, 2 * chan), f32)
    chan_bf = pltpu.HBM((seq_len, chan), bf16)
    sem, sems = pltpu.SemaphoreType.DMA(()), pltpu.SemaphoreType.DMA((count,))
    pairs = pltpu.VMEM((count, INNER, 2 * chan), bf16)
    zs = pltpu.VMEM((count, INNER, 2 * chan), f32)
    turned = pltpu.VMEM((count - 1, INNER, chan), f32)
    one = 8 * count * INNER * INNER * chan

    half = local_t // 2
    steps = chips // 2
    me = lax.axis_index("ctx")

    def to_partner(x):
        return lax.ppermute(x, "ctx", partner)

    def cut(x, start):
        out = jax.ShapeDtypeStruct((half, width), bf16)
        return call(functools.partial(cut_kernel, start), out, 1, flops=half * width)(x)

    def exchange(x):
        return lax.all_to_all(x, "ctx", 0, 0, tiled=True)

    def grad_of(group):
        n = len(group)
        return call(
            functools.partial(grad_kernel, n),
            pltpu.HBM((n * local_t, chan), bf16),
            n + 1,
            flops=2 * n * local_t * width * chan,
        )(*[g[0] for g in group], turned_weight)

    def pair(x, offset, halves=(0, 1)):
        return [(x, offset, 0, halves), (to_partner(x), offset, 1, halves)]

    turned_weight = call(
        turn_kernel, jax.ShapeDtypeStruct((width, chan), bf16), 1, flops=width * chan
    )(out_weight)
    blocks = jax.ShapeDtypeStruct((size, 2, local_t, chan), bf16)
    block = jax.ShapeDtypeStruct((size, local_t, chan), bf16)
    mixed = call(mix_kernel, block, 2, flops=seq_len * chan)(in_hbm(key_rows), in_hbm(value_rows))
    query = call(split_kernel, block, 1, flops=seq_len * chan)(in_hbm(queries_rows))
    mixed = exchange(mixed).reshape(seq_len, chan)
    query = exchange(query).reshape(seq_len, chan)
    filt_spec = call(filter_kernel, spec, 2, [zs, turned, pairs, sems], flops=one, saved=0)(
        in_hbm(filters), table
    )
    groups = [pair(rows, 0)]
    parts = []
    ahead, behind = rows, rows
    for step in range(1, steps):
        ahead = lax.ppermute(ahead, "ctx", forward)
        behind = lax.ppermute(behind, "ctx", backward)
        groups.append(pair(ahead, -step) + pair(behind, step))
        parts.append(grad_of(groups[step - 1]))
    ahead = lax.ppermute(cut(ahead, 0), "ctx", forward)
    behind = lax.ppermute(cut(behind, half), "ctx", backward)
    parts.append(grad_of(groups[-1]))
    conv_chan, mix_spec = call(
        conv_kernel,
        (chan_bf, spec),
        3,
        [zs, zs, zs, pairs, sems, sem],
        flops=2 * one,
        kept=(1,),
        saved=1,
    )(mixed, in_hbm(filt_spec), table)
    groups.append(pair(ahead, -steps, (0,)) + pair(behind, -steps, (1,)))

    where = [[2 * p + h for p in sources(g[1], g[2])] for group in groups for g in group for h in g[3]]
    where = jnp.asarray(np.array(where, np.int32).T)[me]

    def weight_of(members, total, dtype):
        pieces = [g[0] for i in members for g in groups[i]]
        before = sum(len(g[3]) for i in range(members[0]) for g in groups[i])
        units = sum(len(g[3]) for i in members for g in groups[i])
        first = total is None
        return call(
            functools.partial(weight_kernel, len(pieces), first, half),
            jax.ShapeDtypeStruct((chan, width), dtype),
            len(pieces) + 2 + (not first),
            scalars=1,
            flops=2 * units * half * width * chan,
        )(where[before : before + units], *pieces, query, conv_chan, *(() if first else (total,)))

    total = weight_of(range(steps - 1), None, f32)
    total = weight_of([steps - 1], total, f32)
    part_weight = weight_of([steps], total, bf16)
    final = [g[0] for g in groups[-1]]

    back, grad_spec = call(
        functools.partial(tail_kernel, len(parts), len(final)),
        (blocks, spec),
        len(parts) + len(final) + 5,
        [
            pltpu.VMEM((seq_len, chan), bf16),
            pltpu.VMEM((len(final) * half, width), bf16),
            pltpu.VMEM((len(final) * half, chan), bf16),
            zs,
            zs,
            zs,
            pairs,
            sems,
            sem,
        ],
        scalars=1,
        flops=2 * one,
        kept=(len(parts) + len(final) + 3,),
        saved=1,
    )(where, *parts, *final, turned_weight, query, conv_chan, in_hbm(filt_spec), table)
    back = exchange(back)

    taps = call(
        taps_kernel,
        jax.ShapeDtypeStruct((chan, seq_len), bf16),
        3,
        [zs, zs, zs, pairs, turned, pltpu.SemaphoreType.DMA((2,))],
        flops=one,
        kept=(0, 1),
    )(in_hbm(mix_spec), in_hbm(grad_spec), table)
    rows_bf = jax.ShapeDtypeStruct((local_t, size * chan), bf16)
    grad_queries, grad_keys, grad_values = call(
        finish_kernel, (rows_bf, rows_bf, rows_bf), 3, flops=seq_len * chan
    )(back, key_rows, value_rows)

    def over_dp(x):
        n = lax.axis_size("dp")
        total = x.astype(f32)
        if n == 2:
            return total + lax.ppermute(x, "dp", [(0, 1), (1, 0)]).astype(f32)
        return lax.psum(x, "dp").astype(f32)

    return (
        grad_queries[None], grad_keys[None], grad_values[None], over_dp(taps), over_dp(part_weight)
    )


def solution(mesh):
    tokens, chans = P("dp", "ctx", None), P("ctx", None)

    def body(*args):
        return per_device(mesh.shape["ctx"], *args)

    return jax.shard_map(
        body,
        mesh=mesh,
        in_specs=(tokens, tokens, tokens, tokens, chans, chans),
        out_specs=(tokens, tokens, tokens, chans, chans),
        check_vma=False,
    )
```
